256 devices in a mesh: gx: 8 (over y, core), gy: 32 (over z, x).
Axes of the slice: x: 4, y: 4, z: 8, core: 2. Of those that a mesh axis runs over, the one named last changes fastest.
Arguments:
- rhs_values: float32 [32, 524288], P(None, ('gx', 'gy')), may hold values from -6 to 6
- point_coords: float32 [3, 524288], P(None, ('gx', 'gy')), may hold values from 0 to 1, as said below
- leaf_basis: float32 [64, 524288], P(None, ('gx', 'gy')), may hold values from -0.375 to 0.375
- leaf_transfer: float32 [2048, 64, 64], P(('gx', 'gy')), may hold values from -0.75 to 0.75
- cluster_transfer: float32 [256, 64, 64], P(('gx', 'gy')), may hold values from -0.125 to 0.125
- near_list: int32 [2048, 12], P(('gx', 'gy')), may hold values from -1 to 2047, as said below
- coupling_list: int32 [256, 4], P(('gx', 'gy')), may hold values from -1 to 31, as said below
- coupling: float32 [256, 4, 64, 64], P(('gx', 'gy')), may hold values from -0.375 to 0.375
- top_coupling: float32 [8, 8, 64, 64], P('gx'), may hold values from -0.25 to 0.25
Outputs:
- product: float32 [32, 524288], P(None, ('gx', 'gy'))
The draws below stay inside these ranges and needn't reach their ends.
Inputs may be any that keep to these rules, and one draw needn't show every extreme that they name: `near_list`: row t lists distinct leaves that lie within 6 positions of t, t itself first, then the other used entries, then -1 in the unused slots; some leaf uses all 12 slots. `coupling_list`: row d lists distinct positions within the group of cluster d, never the position d % 32 or the ones beside it, used entries first and -1 in the unused slots; some row uses all 4 slots. `point_coords`: the points lie on a closed surface; each leaf's points fill one patch of it, and the leaves follow a Morton order of the patches.
All inputs are finite; a program needn't handle non-finite values.
Results may differ from the reference program's by a relative error of at most 0.0003.
Values sent between devices are 32-bit elements; how exact they have to be, the bound alone decides.
A program may use at most 64 MiB of HBM per device.

```python
import jax
import jax.numpy as jnp
from jax import lax

LEAVES_DEV = 8
LEAF = 256
RANK = 64
RHS = 32
NEAR = 12
REACH = 6
COUP = 4
GROUP_DEVS = 32
GROUPS = 8
CLUSTERS = 256
LEAVES = 2048
POINTS = 524288
N_GX = 8
N_GY = 32


def draw_point_coords(key, part):
    leaves = LEAVES_DEV * N_GX * N_GY
    bit_count = max((leaves - 1).bit_length(), 1)
    major_cells = 2 ** ((bit_count + 1) // 2)
    minor_cells = 2 ** (bit_count // 2)
    leaf_ids = jnp.arange(leaves, dtype=jnp.int32)
    major_index = jnp.zeros((leaves,), jnp.int32)
    minor_index = jnp.zeros((leaves,), jnp.int32)
    for bit in range(bit_count):
        digit = leaf_ids // 2 ** bit % 2
        if bit % 2 == 0:
            major_index = major_index + digit * 2 ** (bit // 2)
        else:
            minor_index = minor_index + digit * 2 ** (bit // 2)
    key_major, key_minor = jax.random.split(jax.random.fold_in(key, 37), 2)
    major_jitter = jax.random.uniform(key_major, (leaves, LEAF), jnp.float32)
    minor_jitter = jax.random.uniform(key_minor, (leaves, LEAF), jnp.float32)
    angle_major = 6.283185307 * (major_index[:, None].astype(jnp.float32) + major_jitter) / major_cells
    angle_minor = 6.283185307 * (minor_index[:, None].astype(jnp.float32) + minor_jitter) / minor_cells
    radial = 0.6 + 0.35 * jnp.cos(angle_minor)
    first = 0.5 + 0.5 * radial * jnp.cos(angle_major)
    second = 0.5 + 0.5 * radial * jnp.sin(angle_major)
    third = 0.5 + 0.5 * 0.35 * jnp.sin(angle_minor)
    stacked = jnp.stack([first, second, third], axis=0)
    return jnp.clip(stacked, 0.0, 1.0).reshape(3, leaves * LEAF).astype(jnp.float32)


def draw_near_list(key, part):
    leaves = LEAVES_DEV * N_GX * N_GY
    devices = N_GX * N_GY
    span_count = 2 * REACH
    key_caps_a, key_caps_b, key_counts, key_shuffle = jax.random.split(jax.random.fold_in(key, 11), 4)
    device_caps = jnp.minimum(jax.random.randint(key_caps_a, (devices,), 2, NEAR + 1), jax.random.randint(key_caps_b, (devices,), 2, NEAR + 1))
    forced = leaves // 2 + REACH
    device_caps = device_caps.at[forced // LEAVES_DEV].set(NEAR)
    cap_rows = jnp.repeat(device_caps, LEAVES_DEV)
    least_count = jnp.maximum(cap_rows // 2, 1)
    counts = least_count + jax.random.randint(key_counts, (leaves,), 0, NEAR + 1) % (cap_rows - least_count + 1)
    counts = counts.at[forced].set(NEAR)
    offset_table = jnp.concatenate([jnp.arange(-REACH, 0, dtype=jnp.int32), jnp.arange(1, REACH + 1, dtype=jnp.int32)])
    shuffles = jax.vmap(lambda one_key: jax.random.permutation(one_key, span_count))(jax.random.split(key_shuffle, leaves))
    candidates = jnp.concatenate([jnp.zeros((leaves, 1), jnp.int32), offset_table[shuffles]], axis=1)
    leaf_ids = jnp.arange(leaves, dtype=jnp.int32)[:, None] + candidates
    inside = (leaf_ids >= 0) & (leaf_ids < leaves)
    sort_keys = jnp.where(inside, 0, span_count + 1) + jnp.arange(span_count + 1, dtype=jnp.int32)[None, :]
    ordering = jnp.argsort(sort_keys, axis=1, stable=True)
    leaf_ids = jnp.take_along_axis(leaf_ids, ordering, axis=1)[:, :NEAR]
    inside = jnp.take_along_axis(inside, ordering, axis=1)[:, :NEAR]
    slot_ids = jnp.arange(NEAR, dtype=jnp.int32)[None, :]
    return jnp.where(inside & (slot_ids < counts[:, None]), leaf_ids, -1).astype(jnp.int32)


def draw_coupling_list(key, part):
    devices = N_GX * N_GY
    key_shuffle, key_counts = jax.random.split(jax.random.fold_in(key, 23), 2)
    shuffles = jax.vmap(lambda one_key: jax.random.permutation(one_key, N_GY))(jax.random.split(key_shuffle, devices))
    own_position = jnp.arange(devices, dtype=jnp.int32) % N_GY
    banned = jnp.abs(shuffles - own_position[:, None]) <= 1
    sort_keys = jnp.where(banned, N_GY, 0) + jnp.arange(N_GY, dtype=jnp.int32)[None, :]
    ordering = jnp.argsort(sort_keys, axis=1, stable=True)
    chosen = jnp.take_along_axis(shuffles, ordering, axis=1)[:, :COUP]
    counts = jax.random.randint(key_counts, (devices,), max(COUP // 2, 1), COUP + 1)
    counts = counts.at[0].set(COUP)
    slot_ids = jnp.arange(COUP, dtype=jnp.int32)[None, :]
    return jnp.where(slot_ids < counts[:, None], chosen, -1).astype(jnp.int32)


def shard_levels(own_key, dims, cuts, low, largest):
    def one(position, blocks):
        heights = jax.random.uniform(jax.random.fold_in(jax.random.fold_in(own_key, 6), position), (blocks,), jnp.float32, low / len(cuts), largest / len(cuts))
        return jnp.repeat(jnp.exp(heights), dims[position] // blocks).reshape((-1,) + (1,) * (len(dims) - position - 1))

    gain = one(*cuts[0])
    for cut in cuts[1:]:
        gain = gain * one(*cut)
    return gain


def bell_draw(key, shape, width, limit, cuts=(), kind=jnp.bfloat16):
    values = width * jax.random.normal(key, shape, jnp.float32)
    if cuts:
        values = values * shard_levels(key, shape, cuts, -0.22, 0.18)
    return jnp.clip(values, -limit, limit).astype(kind)


def setup_inputs(seed: int = 0) -> dict:
    key_list = jax.random.split(jax.random.key(seed), 10)
    rhs_values = bell_draw(key_list[0], (RHS, POINTS), 1.0, 6.0, ((1, 256),), jnp.float32)
    point_coords = draw_point_coords(jax.random.fold_in(key_list[9], 71), 0)
    leaf_basis = bell_draw(key_list[2], (RANK, POINTS), LEAF ** -0.5, 0.375, ((1, 256),), jnp.float32)
    leaf_transfer = bell_draw(key_list[3], (LEAVES, RANK, RANK), RANK ** -0.5, 0.75, ((0, 256),), jnp.float32)
    cluster_transfer = bell_draw(key_list[4], (CLUSTERS, RANK, RANK), (RANK * GROUP_DEVS) ** -0.5, 0.125, ((0, 256),), jnp.float32)
    near_list = draw_near_list(jax.random.fold_in(key_list[9], 71), 0)
    coupling_list = draw_coupling_list(jax.random.fold_in(key_list[9], 71), 0)
    coupling = bell_draw(key_list[7], (CLUSTERS, COUP, RANK, RANK), (RANK * COUP) ** -0.5, 0.375, ((0, 256),), jnp.float32)
    top_coupling = bell_draw(key_list[8], (GROUPS, GROUPS, RANK, RANK), (RANK * GROUPS) ** -0.5, 0.25, ((0, 8),), jnp.float32)
    return {"rhs_values": rhs_values, "point_coords": point_coords, "leaf_basis": leaf_basis, "leaf_transfer": leaf_transfer, "cluster_transfer": cluster_transfer, "near_list": near_list, "coupling_list": coupling_list, "coupling": coupling, "top_coupling": top_coupling}


precise = lax.Precision.HIGHEST
wavenumber = 300.0
softening = 0.0001
core_scale = 0.03

def kernel_tile(targets, sources):
    squared = jnp.zeros(targets.shape[1:2] + (sources.shape[2], targets.shape[2]), targets.dtype)
    for component in range(3):
        gap_part = sources[component][:, :, None] - targets[component][:, None, :]
        squared = squared + gap_part * gap_part
    scale_factor = core_scale * (NEAR * LEAF) ** (-0.5)
    return jnp.cos(wavenumber * jnp.sqrt(squared)) * lax.rsqrt(squared + softening) * scale_factor

def reference(rhs_values, point_coords, leaf_basis, leaf_transfer, cluster_transfer, near_list, coupling_list, coupling, top_coupling):
    leaves = near_list.shape[0]
    clusters = cluster_transfer.shape[0]
    blocks = leaves // LEAVES_DEV
    leaf_values = rhs_values.reshape(RHS, leaves, LEAF)
    leaf_points = point_coords.reshape(3, leaves, LEAF)
    leaf_bases = leaf_basis.reshape(RANK, leaves, LEAF)

    def near_block(block_index):
        block_lists = lax.dynamic_slice_in_dim(near_list, block_index * LEAVES_DEV, LEAVES_DEV, 0)
        targets = lax.dynamic_slice_in_dim(leaf_points, block_index * LEAVES_DEV, LEAVES_DEV, 1)

        def add_slot(slot_index, running):
            column = lax.dynamic_index_in_dim(block_lists, slot_index, 1, keepdims=False)
            usable = column >= 0
            clipped = jnp.where(usable, column, 0).astype(jnp.int32)
            source_vals = jnp.where(usable[None, :, None], jnp.take(leaf_values, clipped, axis=1), 0.0)
            source_pts = jnp.take(leaf_points, clipped, axis=1)
            tile = kernel_tile(targets, source_pts)
            return running + jnp.einsum('rlj,lji->rli', source_vals, tile, precision=precise)
        start = jnp.zeros((RHS, LEAVES_DEV, LEAF), rhs_values.dtype)
        return lax.fori_loop(0, NEAR, add_slot, start)
    near_values = lax.map(near_block, jnp.arange(blocks, dtype=jnp.int32))
    near_values = near_values.transpose(1, 0, 2, 3).reshape(RHS, leaves, LEAF)
    leaf_coeffs = jnp.einsum('rlj,klj->lrk', leaf_values, leaf_bases, precision=precise)
    transfers = leaf_transfer.reshape(clusters, LEAVES_DEV, RANK, RANK)
    cluster_coeffs = jnp.einsum('dlrk,dlkm->drm', leaf_coeffs.reshape(clusters, LEAVES_DEV, RHS, RANK), transfers, precision=precise)
    group_index = jnp.arange(clusters, dtype=jnp.int32) // N_GY
    usable = coupling_list >= 0
    partners = jnp.where(usable, group_index[:, None] * N_GY + coupling_list, 0).astype(jnp.int32)
    selected = jnp.where(usable[:, :, None, None], cluster_coeffs[partners], 0.0)
    coupled = jnp.einsum('dkrm,dkmn->drn', selected, coupling, precision=precise)
    cluster_terms = jnp.einsum('drk,dkm->drm', cluster_coeffs, cluster_transfer, precision=precise)
    group_sums = cluster_terms.reshape(N_GX, N_GY, RHS, RANK).sum(axis=1)
    group_ids = jnp.arange(N_GX, dtype=jnp.int32)
    far_mask = jnp.where(jnp.abs(group_ids[:, None] - group_ids[None, :]) >= 2, 1.0, 0.0).astype(rhs_values.dtype)
    top_field = jnp.einsum('gh,hrk,ghkm->grm', far_mask, group_sums, top_coupling, precision=precise)
    top_each = jnp.repeat(top_field, N_GY, axis=0)
    cluster_field = coupled + jnp.einsum('drm,dkm->drk', top_each, cluster_transfer, precision=precise)
    leaf_field = jnp.einsum('drm,dlkm->dlrk', cluster_field, transfers, precision=precise).reshape(leaves, RHS, RANK)
    far_values = jnp.einsum('lrk,klj->rlj', leaf_field, leaf_bases, precision=precise)
    return (near_values + far_values).reshape(RHS, leaves * LEAF)
```

```python
import functools

import jax
import jax.numpy as jnp
from jax import lax
from jax.experimental import pallas as pl
from jax.experimental.pallas import tpu as pltpu
from jax.sharding import PartitionSpec as P

LEAF = 256
NEAR = 12
REACH = 6
OWN = 8
RHS = 32
RANK = 64
GX = 8
GY = 32
GX_X = 4
GY_Z = 8
TABLE = OWN + REACH
FEAT = 96

F32 = jnp.float32
BF16 = jnp.bfloat16
MESH = pl.DeviceIdType.MESH

TURNS = 300.0 / 6.283185307179586
SOFT = 0.0001 * TURNS * TURNS
C2 = -4.602192823044954
C1 = 9.35955760389501
C0 = -5.69072499925369
D0 = 1.6406295037196048
COS_SCALE = 0.6095221363097632
OUT_SCALE = COS_SCALE * TURNS * 0.03 * (NEAR * LEAF) ** (-0.5)
TINY = 1e-30

FIRST = 22
CROSS = 21
TILES = 56
X_STEP = 7
Z_STEP = 19


def halves(value):
    high = value.astype(BF16)
    low = (value - high.astype(F32)).astype(BF16)
    return high, low


def thirds(value):
    high = value.astype(BF16).astype(F32)
    rest = value - high
    middle = rest.astype(BF16).astype(F32)
    low = (rest - middle).astype(BF16).astype(F32)
    return high, middle, low


def mm(left, right):
    return lax.dot_general(left, right, (((1,), (0,)), ((), ())), preferred_element_type=F32)


def mt(left, right):
    return lax.dot_general(left, right, (((1,), (1,)), ((), ())), preferred_element_type=F32)


def product(left, right, dot):
    left_high, left_low = left
    right_high, right_low = right
    return dot(left_high, right_high) + (dot(left_low, right_high) + dot(left_high, right_low))


def step_at(position, threshold):
    return lax.div(position - threshold + 64, 64)


def pair_of(position):
    position = jnp.minimum(jnp.maximum(position, 0), TILES - 1)
    past_self = step_at(position, OWN)
    past_first = step_at(position, FIRST)
    past_cross = step_at(position, FIRST + CROSS)
    crossing = past_first - past_cross
    other = past_self - crossing
    queue = lax.max(position - OWN - CROSS * past_cross + 4, 0)
    lag = 4 - lax.div(queue, 8)
    own_a = lax.rem(queue, 8)
    own_b = lax.rem(own_a + lag, 8)
    count = position - FIRST
    halo = step_at(count, 6) + step_at(count, 11) + step_at(count, 15) + step_at(count, 18) + step_at(count, 20)
    cross_a = count - lax.div(13 * halo - halo * halo, 2) + halo + 2
    cross_b = OWN + halo
    at_self = 1 - past_self
    a = at_self * position + other * own_a + crossing * cross_a
    b = at_self * position + other * own_b + crossing * cross_b
    return a, b, at_self


def kernel(
    rhs_ref,
    pts_ref,
    basis_ref,
    lt_ref,
    ct_ref,
    near_ref,
    clist_ref,
    coup_ref,
    top_ref,
    out_ref,
    xy_ref,
    centre_ref,
    left_ref,
    vals_ref,
    acc_ref,
    mask_ref,
    base_hi,
    base_lo,
    sq_a,
    sq_b,
    hi_a,
    lo_a,
    hi_b,
    lo_b,
    halo_vals,
    halo_pts,
    halo_list,
    ret_ref,
    x_ref,
    zd_ref,
    zc_ref,
    g_ref,
    halo_send,
    halo_recv,
    meta_send,
    meta_recv,
    ret_send,
    ret_recv,
    x_send,
    x_recv,
    zd_send,
    zd_recv,
    zc_send,
    zc_recv,
    g_send,
    g_recv,
):
    gx = lax.axis_index("gx")
    gy = lax.axis_index("gy")
    x_pos = lax.rem(gy, GX_X)
    z_pos = lax.div(gy, GX_X)
    wrap_up = lax.div(gy + 1, GY)
    wrap_down = lax.div(GY - gy, GY)
    following = (lax.rem(gx + wrap_up, GX), lax.rem(gy + 1, GY))
    previous = (lax.rem(gx + GX - wrap_down, GX), lax.rem(gy + GY - 1, GY))
    x_peers = [(gx, z_pos * GX_X + lax.rem(x_pos + i, GX_X)) for i in range(1, GX_X)]
    z_peers = [(gx, lax.rem(z_pos + i, GY_Z) * GX_X + x_pos) for i in range(1, GY_Z)]
    g_peers = [(lax.rem(gx + i, GX), gy) for i in range(1, GX)]

    def remote(src, dst, send, recv, device):
        return pltpu.make_async_remote_copy(
            src_ref=src, dst_ref=dst, send_sem=send, recv_sem=recv, device_id=device, device_id_type=MESH
        )

    barrier = pltpu.get_barrier_semaphore()
    greeted = [following, previous] + x_peers + z_peers + g_peers
    for device in greeted:
        pl.semaphore_signal(barrier, inc=1, device_id=device, device_id_type=MESH)

    pts_copy = remote(
        pts_ref.at[:, pl.ds(0, REACH * LEAF)], halo_pts, meta_send.at[0], meta_recv.at[0], previous
    )
    list_copy = remote(near_ref, halo_list, meta_send.at[1], meta_recv.at[1], previous)
    halo_copies = [
        remote(
            rhs_ref.at[:, pl.ds(m * LEAF, LEAF)], halo_vals.at[m], halo_send.at[m], halo_recv.at[m], previous
        )
        for m in range(REACH)
    ]
    ret_copies = [
        remote(acc_ref.at[OWN + m], ret_ref.at[m], ret_send.at[m], ret_recv.at[m], following)
        for m in range(REACH)
    ]
    x_copies = [
        remote(x_ref.at[0], x_ref.at[i], x_send.at[i - 1], x_recv.at[i - 1], x_peers[i - 1])
        for i in range(1, GX_X)
    ]
    zd_copies = [
        remote(zd_ref.at[0], zd_ref.at[i], zd_send.at[i - 1], zd_recv.at[i - 1], z_peers[i - 1])
        for i in range(1, GY_Z)
    ]
    zc_copies = [
        remote(zc_ref.at[0], zc_ref.at[i], zc_send.at[i - 1], zc_recv.at[i - 1], z_peers[i - 1])
        for i in range(1, GY_Z)
    ]
    g_copies = [
        remote(g_ref.at[0], g_ref.at[i], g_send.at[i - 1], g_recv.at[i - 1], g_peers[i - 1])
        for i in range(1, GX)
    ]

    first_leaf = (gx * GY + gy) * OWN

    def masks_from(list_value, first):
        rows = first + lax.broadcasted_iota(jnp.int32, (OWN, NEAR), 0)
        used = list_value >= 0
        found = []
        for offset in range(-REACH, REACH + 1):
            hit = jnp.where(used & (list_value == rows + offset), 1.0, 0.0)
            found.append(jnp.broadcast_to(jnp.sum(hit, axis=1, keepdims=True), (OWN, LEAF)))
        return found

    def store_values(slot, value):
        high, low = halves(value)
        vals_ref[slot, 0:RHS, :] = high
        vals_ref[slot, RHS : 2 * RHS, :] = low

    pl.semaphore_wait(barrier, len(greeted))
    pts_copy.start()
    list_copy.start()
    for copy in halo_copies:
        copy.start()

    for t in range(OWN):
        store_values(t, rhs_ref[:, t * LEAF : (t + 1) * LEAF])
    high, low = halves(basis_ref[...])
    base_hi[...] = high
    base_lo[...] = low
    own_coeffs = jnp.zeros((RHS, RANK), F32)
    for t in range(OWN):
        cols = slice(t * LEAF, (t + 1) * LEAF)
        both = mt(vals_ref[t], base_hi[:, cols])
        leaf_coeffs = both[0:RHS] + both[RHS:] + mt(vals_ref[t, 0:RHS, :], base_lo[:, cols])
        own_coeffs = own_coeffs + product(halves(leaf_coeffs), halves(lt_ref[t]), mm)
    own_terms = product(halves(own_coeffs), halves(ct_ref[0]), mm)
    x_ref[0, :, 0:RANK] = own_coeffs
    x_ref[0, :, RANK : 2 * RANK] = own_terms
    for copy in x_copies:
        copy.start()

    xy_ref[...] = jnp.zeros_like(xy_ref)
    for t in range(OWN):
        xy_ref[t, 0:3, :] = pts_ref[:, t * LEAF : (t + 1) * LEAF]
    acc_ref[...] = jnp.zeros_like(acc_ref)
    hi_b[...] = jnp.zeros_like(hi_b)
    lo_b[...] = jnp.zeros_like(lo_b)
    for index, found in enumerate(masks_from(near_ref[...], first_leaf)):
        mask_ref[index, 0:OWN, :] = found
    mask_ref[2 * REACH + 1] = jnp.zeros((2 * OWN, LEAF), F32)
    ones = jnp.ones((8, LEAF), F32)
    for t in range(OWN):
        points = xy_ref[t]
        centre = jnp.broadcast_to(jnp.sum(points, axis=1, keepdims=True) * (1.0 / LEAF), (8, LEAF))
        centre_ref[t] = centre
        high, middle, low = thirds((points - centre) * TURNS)
        whole = (points - centre) * TURNS
        sq_high, sq_middle, sq_low = thirds(whole * whole)
        high, middle, low = -2.0 * high, -2.0 * middle, -2.0 * low
        rows = jnp.concatenate(
            [high, high, middle, middle, high, low, ones, ones, ones, sq_high, sq_middle, sq_low,
             jnp.zeros((128 - FEAT, LEAF), F32)],
            axis=0,
        )
        left_ref[t] = rows.T.astype(BF16)

    def features(a, b):
        whole = (xy_ref[b] - centre_ref[a]) * TURNS
        high, middle, low = thirds(whole)
        sq_high, sq_middle, sq_low = thirds(whole * whole)
        return jnp.concatenate(
            [high, middle, high, middle, low, high, sq_high, sq_middle, sq_low, ones, ones, ones], axis=0
        ).astype(BF16)

    def squares(a, b, into):
        right = features(a, b)
        into[...] = mm(left_ref[a, :, 0:FEAT], right)

    def tile(source, into_hi, into_lo):
        for part in range(4):
            rows = slice(part * 64, part * 64 + 64)
            square = source[rows, :]
            safe = jnp.maximum(square, TINY)
            turns = safe * lax.rsqrt(safe)
            turns = turns - jnp.round(turns)
            q = turns * turns
            cubic = ((q + C2) * q + C1) * q + C0
            wave = D0 - q * (cubic * cubic)
            value = wave * lax.rsqrt(safe + SOFT)
            high = value.astype(BF16)
            into_hi[rows, :] = high
            into_lo[rows, :] = (value - high.astype(F32)).astype(BF16)

    def uses(a, b, at_self, from_hi, from_lo):
        high, low = from_hi[...], from_lo[...]
        offset = b - a
        mask_b = mask_ref[REACH - offset + (REACH + 1 + offset) * at_self, pl.ds(b, 1), :]
        mask_a = mask_ref[REACH + offset, pl.ds(a, 1), :]
        vals_a = vals_ref[a]
        vals_b = vals_ref[b]
        both = mm(vals_a, high)
        sums = both[0:RHS] + both[RHS:] + mm(vals_a[0:RHS], low)
        acc_ref[b] = acc_ref[b] + sums * mask_b
        both = mt(vals_b, high)
        sums = both[0:RHS] + both[RHS:] + mt(vals_b[0:RHS], low)
        acc_ref[a] = acc_ref[a] + sums * mask_a

    def take_meta():
        pts_copy.wait_recv()
        list_copy.wait_recv()
        for m in range(REACH):
            xy_ref[OWN + m, 0:3, :] = halo_pts[:, m * LEAF : (m + 1) * LEAF]
        for index, found in enumerate(masks_from(halo_list[...], first_leaf + OWN)):
            mask_ref[index, OWN : 2 * OWN, :] = found

    def take_values(m):
        halo_copies[m].wait_recv()
        store_values(OWN + m, halo_vals[m])

    def after_x():
        for copy in x_copies:
            copy.wait_recv()
        terms = (x_ref[0] + x_ref[1]) + (x_ref[2] + x_ref[3])
        zd_ref[0] = terms[:, RANK : 2 * RANK]
        for copy in zd_copies:
            copy.start()
        for pair in range(2):
            zc_ref[0, pair] = jnp.concatenate(
                [x_ref[2 * pair, :, 0:RANK], x_ref[2 * pair + 1, :, 0:RANK]], axis=1
            )
        for copy in zc_copies:
            copy.start()

    def after_z():
        for copy in zd_copies:
            copy.wait_recv()
        total = zd_ref[0]
        for i in range(1, GY_Z):
            total = total + zd_ref[i]
        g_ref[0] = total
        for copy in g_copies:
            copy.start()

    squares(0, 0, sq_a)

    def body(it, carry):
        position = it * 2

        def at(when, what):
            pl.when(it == when)(what)

        at(X_STEP, after_x)
        at(Z_STEP, after_z)
        at(10, take_meta)
        for m, when in enumerate((11, 14, 17, 19, 20, 21)):
            at(when, functools.partial(take_values, m))
        for m, when in enumerate((15, 17, 19, 21, 22, 22)):
            at(when, ret_copies[m].start)

        a0, b0, self0 = pair_of(position - 1)
        a1, b1, self1 = pair_of(position)
        a2, b2, _ = pair_of(position + 1)
        a3, b3, _ = pair_of(position + 2)
        squares(a2, b2, sq_b)
        tile(sq_a, hi_a, lo_a)
        uses(a0, b0, self0, hi_b, lo_b)
        squares(a3, b3, sq_a)
        tile(sq_b, hi_b, lo_b)
        uses(a1, b1, self1, hi_a, lo_a)
        return carry

    lax.fori_loop(0, TILES // 2, body, 0)
    a0, b0, self0 = pair_of(jnp.int32(TILES - 1))
    uses(a0, b0, self0, hi_b, lo_b)

    for copy in zc_copies:
        copy.wait_recv()
    coupled = jnp.zeros((RHS, RANK), F32)
    for k in range(4):
        partner = clist_ref[0, k]
        used = jnp.where(partner >= 0, 1.0, 0.0)
        place = jnp.maximum(partner, 0)
        slot_z = lax.rem(z_pos + GY_Z - lax.div(place, GX_X), GY_Z)
        slot_x = lax.rem(x_pos + GX_X - lax.rem(place, GX_X), GX_X)
        row = zc_ref[slot_z, lax.div(slot_x, 2)]
        odd = lax.rem(slot_x, 2).astype(F32)
        chosen = row[:, 0:RANK] * ((1.0 - odd) * used) + row[:, RANK : 2 * RANK] * (odd * used)
        coupled = coupled + product(halves(chosen), halves(coup_ref[0, k]), mm)

    for copy in g_copies:
        copy.wait_recv()
    field = jnp.zeros((RHS, RANK), F32)
    for h in range(GX):
        slot = lax.rem(gx + GX - h, GX)
        gap = lax.max(gx - h, h - gx)
        far = jnp.where(gap >= 2, 1.0, 0.0)
        field = field + product(halves(g_ref[slot] * far), halves(top_ref[0, h]), mm)
    cluster = coupled + product(halves(field), halves(ct_ref[0]), mt)
    cluster = halves(cluster)
    for t in range(OWN):
        cols = slice(t * LEAF, (t + 1) * LEAF)
        leaf_field = product(cluster, halves(lt_ref[t]), mt)
        far_values = product(halves(leaf_field), (base_hi[:, cols], base_lo[:, cols]), mm)
        near_sums = acc_ref[t]
        if t < REACH:
            ret_copies[t].wait_recv()
            near_sums = near_sums + ret_ref[t]
        out_ref[:, cols] = near_sums * OUT_SCALE + far_values

    for copy in [pts_copy, list_copy] + halo_copies + ret_copies + x_copies + zd_copies + zc_copies + g_copies:
        copy.wait_send()


def per_device(*arrays):
    rhs_values = arrays[0]
    vmem = pl.BlockSpec(memory_space=pltpu.VMEM)
    smem = pl.BlockSpec(memory_space=pltpu.SMEM)
    dma = pltpu.SemaphoreType.DMA
    return pl.pallas_call(
        kernel,
        out_shape=jax.ShapeDtypeStruct(rhs_values.shape, F32),
        in_specs=[vmem] * 6 + [smem] + [vmem] * 2,
        out_specs=vmem,
        scratch_shapes=[
            pltpu.VMEM((TABLE, 8, LEAF), F32),
            pltpu.VMEM((OWN, 8, LEAF), F32),
            pltpu.VMEM((OWN, LEAF, 128), BF16),
            pltpu.VMEM((TABLE, 2 * RHS, LEAF), BF16),
            pltpu.VMEM((TABLE, RHS, LEAF), F32),
            pltpu.VMEM((2 * REACH + 2, 2 * OWN, LEAF), F32),
            pltpu.VMEM((RANK, OWN * LEAF), BF16),
            pltpu.VMEM((RANK, OWN * LEAF), BF16),
            pltpu.VMEM((LEAF, LEAF), F32),
            pltpu.VMEM((LEAF, LEAF), F32),
            pltpu.VMEM((LEAF, LEAF), BF16),
            pltpu.VMEM((LEAF, LEAF), BF16),
            pltpu.VMEM((LEAF, LEAF), BF16),
            pltpu.VMEM((LEAF, LEAF), BF16),
            pltpu.VMEM((REACH, RHS, LEAF), F32),
            pltpu.VMEM((3, REACH * LEAF), F32),
            pltpu.VMEM((OWN, NEAR), jnp.int32),
            pltpu.VMEM((REACH, RHS, LEAF), F32),
            pltpu.VMEM((GX_X, RHS, 2 * RANK), F32),
            pltpu.VMEM((GY_Z, RHS, RANK), F32),
            pltpu.VMEM((GY_Z, 2, RHS, 2 * RANK), F32),
            pltpu.VMEM((GX, RHS, RANK), F32),
            dma((REACH,)),
            dma((REACH,)),
            dma((2,)),
            dma((2,)),
            dma((REACH,)),
            dma((REACH,)),
            dma((GX_X - 1,)),
            dma((GX_X - 1,)),
            dma((GY_Z - 1,)),
            dma((GY_Z - 1,)),
            dma((GY_Z - 1,)),
            dma((GY_Z - 1,)),
            dma((GX - 1,)),
            dma((GX - 1,)),
        ],
        compiler_params=pltpu.CompilerParams(collective_id=0, has_side_effects=True),
        name="h2_product",
    )(*arrays)


def solution(mesh):
    return jax.shard_map(
        per_device,
        mesh=mesh,
        in_specs=(
            P(None, ("gx", "gy")),
            P(None, ("gx", "gy")),
            P(None, ("gx", "gy")),
            P(("gx", "gy"), None, None),
            P(("gx", "gy"), None, None),
            P(("gx", "gy"), None),
            P(("gx", "gy"), None),
            P(("gx", "gy"), None, None, None),
            P("gx", None, None, None),
        ),
        out_specs=P(None, ("gx", "gy")),
        check_vma=False,
    )
```

```python
import functools

import jax
import jax.numpy as jnp
from jax import lax
from jax.experimental import pallas as pl
from jax.experimental.pallas import tpu as pltpu
from jax.sharding import PartitionSpec as P

LEAF = 256
NEAR = 12
REACH = 6
OWN = 8
RHS = 32
RANK = 64
GX = 8
GY = 32
GX_X = 4
GY_Z = 8
TABLE = OWN + REACH
FEAT = 96

F32 = jnp.float32
BF16 = jnp.bfloat16
MESH = pl.DeviceIdType.MESH

TURNS = 300.0 / 6.283185307179586
SOFT = 0.0001 * TURNS * TURNS
C2 = -4.602192823044954
C1 = 9.35955760389501
C0 = -5.69072499925369
D0 = 1.6406295037196048
COS_SCALE = 0.6095221363097632
OUT_SCALE = COS_SCALE * TURNS * 0.03 * (NEAR * LEAF) ** (-0.5)
TINY = 1e-30

CROSS = 21
TILES = 56
CROSS_STEP = 12
CROSS_STEP_LATE = 16
X_STEP = 4
Z_STEP = 20
Z_GAP = 4


def halves(value):
    high = value.astype(BF16)
    low = (value - high.astype(F32)).astype(BF16)
    return high, low


def thirds(value):
    high = value.astype(BF16).astype(F32)
    rest = value - high
    middle = rest.astype(BF16).astype(F32)
    low = (rest - middle).astype(BF16).astype(F32)
    return high, middle, low


def mm(left, right):
    return lax.dot_general(left, right, (((1,), (0,)), ((), ())), preferred_element_type=F32)


def mt(left, right):
    return lax.dot_general(left, right, (((1,), (1,)), ((), ())), preferred_element_type=F32)


def product(left, right, dot):
    left_high, left_low = left
    right_high, right_low = right
    return dot(left_high, right_high) + (dot(left_low, right_high) + dot(left_high, right_low))


def step_at(position, threshold):
    return lax.div(position - threshold + 64, 64)


def pair_of(position, first):
    position = jnp.minimum(jnp.maximum(position, 0), TILES - 1)
    past_self = step_at(position, OWN)
    past_first = step_at(position, first)
    past_cross = step_at(position, first + CROSS)
    crossing = past_first - past_cross
    other = past_self - crossing
    queue = lax.max(position - OWN - CROSS * past_cross + 4, 0)
    lag = 4 - lax.div(queue, 8)
    own_a = lax.rem(queue, 8)
    own_b = lax.rem(own_a + lag, 8)
    count = position - first
    halo = step_at(count, 6) + step_at(count, 11) + step_at(count, 15) + step_at(count, 18) + step_at(count, 20)
    cross_a = count - lax.div(13 * halo - halo * halo, 2)
    cross_b = OWN + halo
    at_self = 1 - past_self
    a = at_self * position + other * own_a + crossing * cross_a
    b = at_self * position + other * own_b + crossing * cross_b
    return a, b, at_self, crossing


def kernel(
    rhs_hbm,
    pts_hbm,
    basis_hbm,
    lt_hbm,
    ct_hbm,
    near_hbm,
    clist_ref,
    coup_hbm,
    top_hbm,
    out_ref,
    rhs_ref,
    pts_ref,
    basis_ref,
    lt_ref,
    ct_ref,
    near_ref,
    coup_ref,
    top_ref,
    lt_hi,
    lt_lo,
    top_hi,
    top_lo,
    coup_hi,
    coup_lo,
    load_sem,
    xy_ref,
    centre_ref,
    left_ref,
    vals_ref,
    acc_ref,
    mask_ref,
    base_hi,
    base_lo,
    sq_a,
    sq_b,
    hi_a,
    lo_a,
    hi_b,
    lo_b,
    halo_vals,
    halo_pts,
    halo_list,
    ret_ref,
    x_ref,
    zd_ref,
    zc_ref,
    g_ref,
    halo_send,
    halo_recv,
    meta_send,
    meta_recv,
    ret_send,
    ret_recv,
    x_send,
    x_recv,
    zd_send,
    zd_recv,
    zc_send,
    zc_recv,
    g_send,
    g_recv,
):
    loads = [
        pltpu.make_async_copy(src, dst, load_sem.at[i])
        for i, (src, dst) in enumerate(
            [(rhs_hbm, rhs_ref), (basis_hbm, basis_ref), (lt_hbm, lt_ref), (ct_hbm, ct_ref), (pts_hbm, pts_ref),
             (near_hbm, near_ref), (coup_hbm, coup_ref), (top_hbm, top_ref)]
        )
    ]
    for load in loads:
        load.start()

    gx = lax.axis_index("gx")
    gy = lax.axis_index("gy")
    x_pos = lax.rem(gy, GX_X)
    z_pos = lax.div(gy, GX_X)
    wrap_up = lax.div(gy + 1, GY)
    wrap_down = lax.div(GY - gy, GY)
    following = (lax.rem(gx + wrap_up, GX), lax.rem(gy + 1, GY))
    previous = (lax.rem(gx + GX - wrap_down, GX), lax.rem(gy + GY - 1, GY))
    x_peers = [(gx, z_pos * GX_X + lax.rem(x_pos + i, GX_X)) for i in range(1, GX_X)]
    z_peers = [(gx, lax.rem(z_pos + i, GY_Z) * GX_X + x_pos) for i in range(1, GY_Z)]
    g_peers = [(lax.rem(gx + i, GX), gy) for i in range(1, GX)]

    def remote(src, dst, send, recv, device):
        return pltpu.make_async_remote_copy(
            src_ref=src, dst_ref=dst, send_sem=send, recv_sem=recv, device_id=device, device_id_type=MESH
        )

    barrier = pltpu.get_barrier_semaphore()
    greeted = [previous] + x_peers + g_peers
    for device in greeted:
        pl.semaphore_signal(barrier, inc=1, device_id=device, device_id_type=MESH)
    for i in range(1, GY_Z):

        @pl.when(z_pos + i < GY_Z)
        def _(i=i):
            pl.semaphore_signal(barrier, inc=1, device_id=z_peers[i - 1], device_id_type=MESH)

    pts_copy = remote(
        pts_ref.at[:, pl.ds(2 * LEAF, REACH * LEAF)], halo_pts, meta_send.at[0], meta_recv.at[0], following
    )
    list_copy = remote(near_ref, halo_list, meta_send.at[1], meta_recv.at[1], following)
    halo_copies = [
        remote(
            rhs_ref.at[:, pl.ds((OWN - 1 - m) * LEAF, LEAF)],
            halo_vals.at[m],
            halo_send.at[m],
            halo_recv.at[m],
            following,
        )
        for m in range(REACH)
    ]
    ret_copies = [
        remote(acc_ref.at[OWN + m], ret_ref.at[m], ret_send.at[m], ret_recv.at[m], previous)
        for m in range(REACH)
    ]
    x_copies = [
        remote(x_ref.at[0], x_ref.at[i], x_send.at[i - 1], x_recv.at[i - 1], x_peers[i - 1])
        for i in range(1, GX_X)
    ]
    zd_copies = [
        remote(zd_ref.at[0], zd_ref.at[i], zd_send.at[i - 1], zd_recv.at[i - 1], z_peers[i - 1])
        for i in range(1, GY_Z)
    ]
    zc_copies = [
        remote(zc_ref.at[0], zc_ref.at[i], zc_send.at[i - 1], zc_recv.at[i - 1], z_peers[i - 1])
        for i in range(1, GY_Z)
    ]
    g_copies = [
        remote(g_ref.at[0], g_ref.at[i], g_send.at[i - 1], g_recv.at[i - 1], g_peers[i - 1])
        for i in range(1, GX)
    ]

    first_leaf = (gx * GY + gy) * OWN

    def masks_from(list_value, first):
        rows = first + lax.broadcasted_iota(jnp.int32, (OWN, NEAR), 0)
        used = list_value >= 0
        found = []
        for offset in range(-REACH, REACH + 1):
            hit = jnp.where(used & (list_value == rows + offset), 1.0, 0.0)
            found.append(jnp.broadcast_to(jnp.sum(hit, axis=1, keepdims=True), (OWN, LEAF)))
        return found

    def store_values(slot, value):
        high, low = halves(value)
        vals_ref[slot, 0:RHS, :] = high
        vals_ref[slot, RHS : 2 * RHS, :] = low

    loads[0].wait()
    for t in range(OWN):
        store_values(t, rhs_ref[:, t * LEAF : (t + 1) * LEAF])
    loads[1].wait()
    high, low = halves(basis_ref[...])
    base_hi[...] = high
    base_lo[...] = low
    loads[2].wait()
    high, low = halves(lt_ref[...])
    lt_hi[...] = high
    lt_lo[...] = low
    own_coeffs = jnp.zeros((RHS, RANK), F32)
    for t in range(OWN):
        cols = slice(t * LEAF, (t + 1) * LEAF)
        both = mt(vals_ref[t], base_hi[:, cols])
        leaf_coeffs = both[0:RHS] + both[RHS:] + mt(vals_ref[t, 0:RHS, :], base_lo[:, cols])
        own_coeffs = own_coeffs + product(halves(leaf_coeffs), (lt_hi[t], lt_lo[t]), mm)
    loads[3].wait()
    own_terms = product(halves(own_coeffs), halves(ct_ref[0]), mm)
    x_ref[0, :, 0:RANK] = own_coeffs
    x_ref[0, :, RANK : 2 * RANK] = own_terms
    loads[4].wait()
    loads[5].wait()
    pl.semaphore_wait(barrier, len(greeted) + z_pos)
    for copy in x_copies:
        copy.start()
    pts_copy.start()
    list_copy.start()
    for copy in halo_copies:
        copy.start()

    xy_ref[...] = jnp.zeros_like(xy_ref)
    for t in range(OWN):
        xy_ref[t, 0:3, :] = pts_ref[:, t * LEAF : (t + 1) * LEAF]
    acc_ref[...] = jnp.zeros_like(acc_ref)
    hi_b[...] = jnp.zeros_like(hi_b)
    lo_b[...] = jnp.zeros_like(lo_b)
    for index, found in enumerate(masks_from(near_ref[...], first_leaf)):
        mask_ref[index, 0:OWN, :] = found
    mask_ref[2 * REACH + 1] = jnp.zeros((2 * OWN, LEAF), F32)
    ones = jnp.ones((8, LEAF), F32)
    for t in range(OWN):
        points = xy_ref[t]
        centre = jnp.broadcast_to(jnp.sum(points, axis=1, keepdims=True) * (1.0 / LEAF), (8, LEAF))
        centre_ref[t] = centre
        high, middle, low = thirds((points - centre) * TURNS)
        whole = (points - centre) * TURNS
        sq_high, sq_middle, sq_low = thirds(whole * whole)
        high, middle, low = -2.0 * high, -2.0 * middle, -2.0 * low
        rows = jnp.concatenate(
            [high, high, middle, middle, high, low, ones, ones, ones, sq_high, sq_middle, sq_low,
             jnp.zeros((128 - FEAT, LEAF), F32)],
            axis=0,
        )
        left_ref[t] = rows.T.astype(BF16)

    def features(a, b):
        whole = (xy_ref[b] - centre_ref[a]) * TURNS
        high, middle, low = thirds(whole)
        sq_high, sq_middle, sq_low = thirds(whole * whole)
        return jnp.concatenate(
            [high, middle, high, middle, low, high, sq_high, sq_middle, sq_low, ones, ones, ones], axis=0
        ).astype(BF16)

    def squares(a, b, into):
        right = features(a, b)
        into[...] = mm(left_ref[a, :, 0:FEAT], right)

    def tile(source, into_hi, into_lo):
        for part in range(4):
            rows = slice(part * 64, part * 64 + 64)
            square = source[rows, :]
            safe = jnp.maximum(square, TINY)
            turns = safe * lax.rsqrt(safe)
            turns = turns - jnp.round(turns)
            q = turns * turns
            cubic = ((q + C2) * q + C1) * q + C0
            wave = D0 - q * (cubic * cubic)
            value = wave * lax.rsqrt(safe + SOFT)
            high = value.astype(BF16)
            into_hi[rows, :] = high
            into_lo[rows, :] = (value - high.astype(F32)).astype(BF16)

    def uses(pair, from_hi, from_lo):
        a, b, at_self, crossing = pair
        high, low = from_hi[...], from_lo[...]
        offset = (1 - crossing) * (b - a) + crossing * (OWN - 1 - b - a)
        row = (1 - crossing) * b + crossing * (3 * OWN - 1 - b)
        mask_b = mask_ref[REACH - offset + (REACH + 1 + offset) * at_self, pl.ds(row, 1), :]
        mask_a = mask_ref[REACH + offset, pl.ds(a, 1), :]
        vals_a = vals_ref[a]
        vals_b = vals_ref[b]
        both = mm(vals_a, high)
        sums = both[0:RHS] + both[RHS:] + mm(vals_a[0:RHS], low)
        acc_ref[b] = acc_ref[b] + sums * mask_b
        both = mt(vals_b, high)
        sums = both[0:RHS] + both[RHS:] + mt(vals_b[0:RHS], low)
        acc_ref[a] = acc_ref[a] + sums * mask_a

    def take_meta():
        pts_copy.wait_recv()
        list_copy.wait_recv()
        for m in range(REACH):
            cols = slice((REACH - 1 - m) * LEAF, (REACH - m) * LEAF)
            xy_ref[OWN + m, 0:3, :] = halo_pts[:, cols]
        for index, found in enumerate(masks_from(halo_list[...], first_leaf - OWN)):
            mask_ref[index, OWN : 2 * OWN, :] = found

    def take_values(m):
        halo_copies[m].wait_recv()
        store_values(OWN + m, halo_vals[m])

    def after_x():
        for copy in x_copies:
            copy.wait_recv()
        terms = (x_ref[0] + x_ref[1]) + (x_ref[2] + x_ref[3])
        zd_ref[0] = terms[:, RANK : 2 * RANK]
        for pair in range(2):
            zc_ref[0, pair] = jnp.concatenate(
                [x_ref[2 * pair, :, 0:RANK], x_ref[2 * pair + 1, :, 0:RANK]], axis=1
            )
        for copies in (zd_copies, zc_copies):
            for i in range(1, GY_Z):
                pl.when(z_pos + i >= GY_Z)(copies[i - 1].start)

    def after_high():
        for i in range(1, GY_Z):
            pl.when(i > z_pos)(zd_copies[i - 1].wait_recv)
        for copies in (zd_copies, zc_copies):
            for i in range(1, GY_Z):
                pl.when(z_pos + i < GY_Z)(copies[i - 1].start)

    def after_low():
        for i in range(1, GY_Z):
            pl.when(i <= z_pos)(zd_copies[i - 1].wait_recv)
        total = zd_ref[0]
        for i in range(1, GY_Z):
            total = total + zd_ref[i]
        g_ref[0] = total
        for copy in g_copies:
            copy.start()

    late = lax.div(GY - gy, GY)
    cross_step = CROSS_STEP + (CROSS_STEP_LATE - CROSS_STEP) * late
    first = 2 * cross_step
    high_step = Z_STEP - lax.div(7 * z_pos, 4)
    low_step = high_step + Z_GAP

    squares(0, 0, sq_a)

    def body(it, carry):
        position = it * 2

        def at(when, what):
            pl.when(it == when)(what)

        at(X_STEP, after_x)
        at(high_step, after_high)
        at(low_step, after_low)
        at(cross_step - 1, take_meta)
        for m, after in enumerate((0, 3, 6, 8, 9, 10)):
            at(cross_step + after, functools.partial(take_values, m))
        for m, after in enumerate((4, 6, 8, 10, 11, 11)):
            at(cross_step + after, ret_copies[m].start)

        before, this = pair_of(position - 1, first), pair_of(position, first)
        second, third = pair_of(position + 1, first), pair_of(position + 2, first)
        squares(second[0], second[1], sq_b)
        tile(sq_a, hi_a, lo_a)
        uses(before, hi_b, lo_b)
        squares(third[0], third[1], sq_a)
        tile(sq_b, hi_b, lo_b)
        uses(this, hi_a, lo_a)
        return carry

    lax.fori_loop(0, TILES // 2, body, 0)
    uses(pair_of(jnp.int32(TILES - 1), first), hi_b, lo_b)

    loads[6].wait()
    loads[7].wait()
    top_hi[...], top_lo[...] = halves(top_ref[0])
    coup_hi[...], coup_lo[...] = halves(coup_ref[0])
    ct_halves = halves(ct_ref[0])
    for copy in zc_copies:
        copy.wait_recv()
    coupled = jnp.zeros((RHS, RANK), F32)
    for k in range(4):
        partner = clist_ref[0, k]
        used = jnp.where(partner >= 0, 1.0, 0.0)
        place = jnp.maximum(partner, 0)
        slot_z = lax.rem(z_pos + GY_Z - lax.div(place, GX_X), GY_Z)
        slot_x = lax.rem(x_pos + GX_X - lax.rem(place, GX_X), GX_X)
        row = zc_ref[slot_z, lax.div(slot_x, 2)]
        odd = lax.rem(slot_x, 2).astype(F32)
        chosen = row[:, 0:RANK] * ((1.0 - odd) * used) + row[:, RANK : 2 * RANK] * (odd * used)
        coupled = coupled + product(halves(chosen), (coup_hi[k], coup_lo[k]), mm)

    for copy in g_copies:
        copy.wait_recv()
    field = jnp.zeros((RHS, RANK), F32)
    for h in range(GX):
        slot = lax.rem(gx + GX - h, GX)
        gap = lax.max(gx - h, h - gx)
        far = jnp.where(gap >= 2, 1.0, 0.0)
        field = field + product(halves(g_ref[slot] * far), (top_hi[h], top_lo[h]), mm)
    cluster = coupled + product(halves(field), ct_halves, mt)
    cluster = halves(cluster)
    for t in range(OWN):
        cols = slice(t * LEAF, (t + 1) * LEAF)
        leaf_field = product(cluster, (lt_hi[t], lt_lo[t]), mt)
        far_values = product(halves(leaf_field), (base_hi[:, cols], base_lo[:, cols]), mm)
        near_sums = acc_ref[t]
        if t >= OWN - REACH:
            ret_copies[OWN - 1 - t].wait_recv()
            near_sums = near_sums + ret_ref[OWN - 1 - t]
        out_ref[:, cols] = near_sums * OUT_SCALE + far_values

    for copy in [pts_copy, list_copy] + halo_copies + ret_copies + x_copies + zd_copies + zc_copies + g_copies:
        copy.wait_send()


def per_device(*arrays):
    rhs_values = arrays[0]
    vmem = pl.BlockSpec(memory_space=pltpu.VMEM)
    anywhere = pl.BlockSpec(memory_space=pl.ANY)
    smem = pl.BlockSpec(memory_space=pltpu.SMEM)
    dma = pltpu.SemaphoreType.DMA
    return pl.pallas_call(
        kernel,
        out_shape=jax.ShapeDtypeStruct(rhs_values.shape, F32),
        in_specs=[anywhere] * 6 + [smem] + [anywhere] * 2,
        out_specs=vmem,
        scratch_shapes=[
            pltpu.VMEM((RHS, OWN * LEAF), F32),
            pltpu.VMEM((3, OWN * LEAF), F32),
            pltpu.VMEM((RANK, OWN * LEAF), F32),
            pltpu.VMEM((OWN, RANK, RANK), F32),
            pltpu.VMEM((1, RANK, RANK), F32),
            pltpu.VMEM((OWN, NEAR), jnp.int32),
            pltpu.VMEM((1, 4, RANK, RANK), F32),
            pltpu.VMEM((1, GX, RANK, RANK), F32),
            pltpu.VMEM((OWN, RANK, RANK), BF16),
            pltpu.VMEM((OWN, RANK, RANK), BF16),
            pltpu.VMEM((GX, RANK, RANK), BF16),
            pltpu.VMEM((GX, RANK, RANK), BF16),
            pltpu.VMEM((4, RANK, RANK), BF16),
            pltpu.VMEM((4, RANK, RANK), BF16),
            dma((8,)),
            pltpu.VMEM((TABLE, 8, LEAF), F32),
            pltpu.VMEM((OWN, 8, LEAF), F32),
            pltpu.VMEM((OWN, LEAF, 128), BF16),
            pltpu.VMEM((TABLE, 2 * RHS, LEAF), BF16),
            pltpu.VMEM((TABLE, RHS, LEAF), F32),
            pltpu.VMEM((2 * REACH + 2, 2 * OWN, LEAF), F32),
            pltpu.VMEM((RANK, OWN * LEAF), BF16),
            pltpu.VMEM((RANK, OWN * LEAF), BF16),
            pltpu.VMEM((LEAF, LEAF), F32),
            pltpu.VMEM((LEAF, LEAF), F32),
            pltpu.VMEM((LEAF, LEAF), BF16),
            pltpu.VMEM((LEAF, LEAF), BF16),
            pltpu.VMEM((LEAF, LEAF), BF16),
            pltpu.VMEM((LEAF, LEAF), BF16),
            pltpu.VMEM((REACH, RHS, LEAF), F32),
            pltpu.VMEM((3, REACH * LEAF), F32),
            pltpu.VMEM((OWN, NEAR), jnp.int32),
            pltpu.VMEM((REACH, RHS, LEAF), F32),
            pltpu.VMEM((GX_X, RHS, 2 * RANK), F32),
            pltpu.VMEM((GY_Z, RHS, RANK), F32),
            pltpu.VMEM((GY_Z, 2, RHS, 2 * RANK), F32),
            pltpu.VMEM((GX, RHS, RANK), F32),
            dma((REACH,)),
            dma((REACH,)),
            dma((2,)),
            dma((2,)),
            dma((REACH,)),
            dma((REACH,)),
            dma((GX_X - 1,)),
            dma((GX_X - 1,)),
            dma((GY_Z - 1,)),
            dma((GY_Z - 1,)),
            dma((GY_Z - 1,)),
            dma((GY_Z - 1,)),
            dma((GX - 1,)),
            dma((GX - 1,)),
        ],
        compiler_params=pltpu.CompilerParams(collective_id=0, has_side_effects=True),
        name="h2_product",
    )(*arrays)


def solution(mesh):
    return jax.shard_map(
        per_device,
        mesh=mesh,
        in_specs=(
            P(None, ("gx", "gy")),
            P(None, ("gx", "gy")),
            P(None, ("gx", "gy")),
            P(("gx", "gy"), None, None),
            P(("gx", "gy"), None, None),
            P(("gx", "gy"), None),
            P(("gx", "gy"), None),
            P(("gx", "gy"), None, None, None),
            P("gx", None, None, None),
        ),
        out_specs=P(None, ("gx", "gy")),
        check_vma=False,
    )
```

```python
import functools

import jax
import jax.numpy as jnp
from jax import lax
from jax.experimental import pallas as pl
from jax.experimental.pallas import tpu as pltpu
from jax.sharding import PartitionSpec as P

LEAF = 256
NEAR = 12
REACH = 6
OWN = 8
RHS = 32
RANK = 64
GX = 8
GY = 32
GX_X = 4
GY_Z = 8
TABLE = OWN + REACH
FEAT = 96

F32 = jnp.float32
BF16 = jnp.bfloat16
MESH = pl.DeviceIdType.MESH

TURNS = 300.0 / 6.283185307179586
SOFT = 0.0001 * TURNS * TURNS
C2 = -4.602192823044954
C1 = 9.35955760389501
C0 = -5.69072499925369
D0 = 1.6406295037196048
COS_SCALE = 0.6095221363097632
OUT_SCALE = COS_SCALE * TURNS * 0.03 * (NEAR * LEAF) ** (-0.5)
TINY = 1e-30

CROSS = 21
TILES = 56
CROSS_STEP = 11
CROSS_STEP_LATE = 16
HIGH_STEP = 14
LOW_STEP = 16
X_STEP = 22


def halves(value):
    high = value.astype(BF16)
    low = (value - high.astype(F32)).astype(BF16)
    return high, low


def thirds(value):
    high = value.astype(BF16).astype(F32)
    rest = value - high
    middle = rest.astype(BF16).astype(F32)
    low = (rest - middle).astype(BF16).astype(F32)
    return high, middle, low


def mm(left, right):
    return lax.dot_general(left, right, (((1,), (0,)), ((), ())), preferred_element_type=F32)


def mt(left, right):
    return lax.dot_general(left, right, (((1,), (1,)), ((), ())), preferred_element_type=F32)


def product(left, right, dot):
    left_high, left_low = left
    right_high, right_low = right
    return dot(left_high, right_high) + (dot(left_low, right_high) + dot(left_high, right_low))


def step_at(position, threshold):
    return lax.div(position - threshold + 64, 64)


def pair_of(position, first):
    position = jnp.minimum(jnp.maximum(position, 0), TILES - 1)
    past_self = step_at(position, OWN)
    past_first = step_at(position, first)
    past_cross = step_at(position, first + CROSS)
    crossing = past_first - past_cross
    other = past_self - crossing
    queue = lax.max(position - OWN - CROSS * past_cross + 4, 0)
    lag = 4 - lax.div(queue, 8)
    own_a = lax.rem(queue, 8)
    own_b = lax.rem(own_a + lag, 8)
    count = position - first
    halo = step_at(count, 6) + step_at(count, 11) + step_at(count, 15) + step_at(count, 18) + step_at(count, 20)
    cross_a = count - lax.div(13 * halo - halo * halo, 2)
    cross_b = OWN + halo
    at_self = 1 - past_self
    a = at_self * position + other * own_a + crossing * cross_a
    b = at_self * position + other * own_b + crossing * cross_b
    return a, b, at_self, crossing


def kernel(
    rhs_hbm,
    pts_hbm,
    basis_hbm,
    lt_hbm,
    ct_hbm,
    near_hbm,
    clist_ref,
    coup_hbm,
    top_hbm,
    out_ref,
    rhs_ref,
    pts_ref,
    basis_ref,
    lt_ref,
    ct_ref,
    near_ref,
    coup_ref,
    top_ref,
    lt_hi,
    lt_lo,
    top_hi,
    top_lo,
    coup_hi,
    coup_lo,
    load_sem,
    xy_ref,
    centre_ref,
    left_ref,
    vals_ref,
    acc_ref,
    mask_ref,
    base_hi,
    base_lo,
    sq_a,
    sq_b,
    hi_a,
    lo_a,
    hi_b,
    lo_b,
    halo_vals,
    halo_pts,
    halo_list,
    ret_ref,
    z_ref,
    xd_ref,
    xc_ref,
    g_ref,
    halo_send,
    halo_recv,
    meta_send,
    meta_recv,
    ret_send,
    ret_recv,
    z_send,
    z_recv,
    xd_send,
    xd_recv,
    xc_send,
    xc_recv,
    g_send,
    g_recv,
):
    loads = [
        pltpu.make_async_copy(src, dst, load_sem.at[i])
        for i, (src, dst) in enumerate(
            [(rhs_hbm, rhs_ref), (basis_hbm, basis_ref), (lt_hbm, lt_ref), (ct_hbm, ct_ref), (pts_hbm, pts_ref),
             (near_hbm, near_ref), (coup_hbm, coup_ref), (top_hbm, top_ref)]
        )
    ]
    for load in loads:
        load.start()

    gx = lax.axis_index("gx")
    gy = lax.axis_index("gy")
    x_pos = lax.rem(gy, GX_X)
    z_pos = lax.div(gy, GX_X)
    wrap_up = lax.div(gy + 1, GY)
    wrap_down = lax.div(GY - gy, GY)
    following = (lax.rem(gx + wrap_up, GX), lax.rem(gy + 1, GY))
    previous = (lax.rem(gx + GX - wrap_down, GX), lax.rem(gy + GY - 1, GY))
    x_peers = [(gx, z_pos * GX_X + lax.rem(x_pos + i, GX_X)) for i in range(1, GX_X)]
    z_peers = [(gx, lax.rem(z_pos + i, GY_Z) * GX_X + x_pos) for i in range(1, GY_Z)]
    g_peers = [(lax.rem(gx + i, GX), gy) for i in range(1, GX)]

    def remote(src, dst, send, recv, device):
        return pltpu.make_async_remote_copy(
            src_ref=src, dst_ref=dst, send_sem=send, recv_sem=recv, device_id=device, device_id_type=MESH
        )

    barrier = pltpu.get_barrier_semaphore()
    greeted = [previous] + x_peers + g_peers
    for device in greeted:
        pl.semaphore_signal(barrier, inc=1, device_id=device, device_id_type=MESH)
    for i in range(1, GY_Z):

        @pl.when(z_pos + i < GY_Z)
        def _(i=i):
            pl.semaphore_signal(barrier, inc=1, device_id=z_peers[i - 1], device_id_type=MESH)

    pts_copy = remote(
        pts_ref.at[:, pl.ds(2 * LEAF, REACH * LEAF)], halo_pts, meta_send.at[0], meta_recv.at[0], following
    )
    list_copy = remote(near_ref, halo_list, meta_send.at[1], meta_recv.at[1], following)
    halo_copies = [
        remote(
            rhs_ref.at[:, pl.ds((OWN - 1 - m) * LEAF, LEAF)],
            halo_vals.at[m],
            halo_send.at[m],
            halo_recv.at[m],
            following,
        )
        for m in range(REACH)
    ]
    ret_copies = [
        remote(acc_ref.at[OWN + m], ret_ref.at[m], ret_send.at[m], ret_recv.at[m], previous)
        for m in range(REACH)
    ]
    z_copies = [
        remote(z_ref.at[0], z_ref.at[i], z_send.at[i - 1], z_recv.at[i - 1], z_peers[i - 1])
        for i in range(1, GY_Z)
    ]
    xd_copies = [
        remote(xd_ref.at[0], xd_ref.at[i], xd_send.at[i - 1], xd_recv.at[i - 1], x_peers[i - 1])
        for i in range(1, GX_X)
    ]
    xc_copies = [
        remote(xc_ref.at[0], xc_ref.at[i], xc_send.at[i - 1], xc_recv.at[i - 1], x_peers[i - 1])
        for i in range(1, GX_X)
    ]
    g_copies = [
        remote(g_ref.at[0], g_ref.at[i], g_send.at[i - 1], g_recv.at[i - 1], g_peers[i - 1])
        for i in range(1, GX)
    ]

    first_leaf = (gx * GY + gy) * OWN

    def masks_from(list_value, first):
        rows = first + lax.broadcasted_iota(jnp.int32, (OWN, NEAR), 0)
        used = list_value >= 0
        found = []
        for offset in range(-REACH, REACH + 1):
            hit = jnp.where(used & (list_value == rows + offset), 1.0, 0.0)
            found.append(jnp.broadcast_to(jnp.sum(hit, axis=1, keepdims=True), (OWN, LEAF)))
        return found

    def store_values(slot, value):
        high, low = halves(value)
        vals_ref[slot, 0:RHS, :] = high
        vals_ref[slot, RHS : 2 * RHS, :] = low

    loads[0].wait()
    for t in range(OWN):
        store_values(t, rhs_ref[:, t * LEAF : (t + 1) * LEAF])
    loads[1].wait()
    high, low = halves(basis_ref[...])
    base_hi[...] = high
    base_lo[...] = low
    loads[2].wait()
    high, low = halves(lt_ref[...])
    lt_hi[...] = high
    lt_lo[...] = low
    own_coeffs = jnp.zeros((RHS, RANK), F32)
    for t in range(OWN):
        cols = slice(t * LEAF, (t + 1) * LEAF)
        both = mt(vals_ref[t], base_hi[:, cols])
        leaf_coeffs = both[0:RHS] + both[RHS:] + mt(vals_ref[t, 0:RHS, :], base_lo[:, cols])
        own_coeffs = own_coeffs + product(halves(leaf_coeffs), (lt_hi[t], lt_lo[t]), mm)
    loads[3].wait()
    own_terms = product(halves(own_coeffs), halves(ct_ref[0]), mm)
    z_ref[0, :, 0:RANK] = own_coeffs
    z_ref[0, :, RANK : 2 * RANK] = own_terms
    loads[4].wait()
    loads[5].wait()

    def begin():
        pl.semaphore_wait(barrier, len(greeted) + z_pos)
        for i in range(1, GY_Z):
            pl.when(z_pos + i >= GY_Z)(z_copies[i - 1].start)
        pts_copy.start()
        list_copy.start()
        for copy in halo_copies:
            copy.start()

    xy_ref[...] = jnp.zeros_like(xy_ref)
    for t in range(OWN):
        xy_ref[t, 0:3, :] = pts_ref[:, t * LEAF : (t + 1) * LEAF]
    acc_ref[...] = jnp.zeros_like(acc_ref)
    hi_b[...] = jnp.zeros_like(hi_b)
    lo_b[...] = jnp.zeros_like(lo_b)
    for index, found in enumerate(masks_from(near_ref[...], first_leaf)):
        mask_ref[index, 0:OWN, :] = found
    mask_ref[2 * REACH + 1] = jnp.zeros((2 * OWN, LEAF), F32)
    ones = jnp.ones((8, LEAF), F32)
    for t in range(OWN):
        points = xy_ref[t]
        centre = jnp.broadcast_to(jnp.sum(points, axis=1, keepdims=True) * (1.0 / LEAF), (8, LEAF))
        centre_ref[t] = centre
        high, middle, low = thirds((points - centre) * TURNS)
        whole = (points - centre) * TURNS
        sq_high, sq_middle, sq_low = thirds(whole * whole)
        high, middle, low = -2.0 * high, -2.0 * middle, -2.0 * low
        rows = jnp.concatenate(
            [high, high, middle, middle, high, low, ones, ones, ones, sq_high, sq_middle, sq_low,
             jnp.zeros((128 - FEAT, LEAF), F32)],
            axis=0,
        )
        left_ref[t] = rows.T.astype(BF16)

    def features(a, b):
        whole = (xy_ref[b] - centre_ref[a]) * TURNS
        high, middle, low = thirds(whole)
        sq_high, sq_middle, sq_low = thirds(whole * whole)
        return jnp.concatenate(
            [high, middle, high, middle, low, high, sq_high, sq_middle, sq_low, ones, ones, ones], axis=0
        ).astype(BF16)

    def squares(a, b, into):
        right = features(a, b)
        into[...] = mm(left_ref[a, :, 0:FEAT], right)

    def tile(source, into_hi, into_lo):
        for part in range(4):
            rows = slice(part * 64, part * 64 + 64)
            square = source[rows, :]
            safe = jnp.maximum(square, TINY)
            turns = safe * lax.rsqrt(safe)
            turns = turns - jnp.round(turns)
            q = turns * turns
            cubic = ((q + C2) * q + C1) * q + C0
            wave = D0 - q * (cubic * cubic)
            value = wave * lax.rsqrt(safe + SOFT)
            high = value.astype(BF16)
            into_hi[rows, :] = high
            into_lo[rows, :] = (value - high.astype(F32)).astype(BF16)

    def uses(pair, from_hi, from_lo):
        a, b, at_self, crossing = pair
        high, low = from_hi[...], from_lo[...]
        offset = (1 - crossing) * (b - a) + crossing * (OWN - 1 - b - a)
        row = (1 - crossing) * b + crossing * (3 * OWN - 1 - b)
        mask_b = mask_ref[REACH - offset + (REACH + 1 + offset) * at_self, pl.ds(row, 1), :]
        mask_a = mask_ref[REACH + offset, pl.ds(a, 1), :]
        vals_a = vals_ref[a]
        vals_b = vals_ref[b]
        both = mm(vals_a, high)
        sums = both[0:RHS] + both[RHS:] + mm(vals_a[0:RHS], low)
        acc_ref[b] = acc_ref[b] + sums * mask_b
        both = mt(vals_b, high)
        sums = both[0:RHS] + both[RHS:] + mt(vals_b[0:RHS], low)
        acc_ref[a] = acc_ref[a] + sums * mask_a

    def take_meta():
        pts_copy.wait_recv()
        list_copy.wait_recv()
        for m in range(REACH):
            cols = slice((REACH - 1 - m) * LEAF, (REACH - m) * LEAF)
            xy_ref[OWN + m, 0:3, :] = halo_pts[:, cols]
        for index, found in enumerate(masks_from(halo_list[...], first_leaf - OWN)):
            mask_ref[index, OWN : 2 * OWN, :] = found

    def take_values(m):
        halo_copies[m].wait_recv()
        store_values(OWN + m, halo_vals[m])

    def after_high():
        for i in range(1, GY_Z):
            pl.when(i > z_pos)(z_copies[i - 1].wait_recv)
        for i in range(1, GY_Z):
            pl.when(z_pos + i < GY_Z)(z_copies[i - 1].start)

    def after_low():
        for i in range(1, GY_Z):
            pl.when(i <= z_pos)(z_copies[i - 1].wait_recv)
        terms = z_ref[0, :, RANK : 2 * RANK]
        for i in range(1, GY_Z):
            terms = terms + z_ref[i, :, RANK : 2 * RANK]
        half = RHS // 2
        xd_ref[0] = jnp.concatenate([terms[0:half], terms[half:]], axis=1)
        for copy in xd_copies:
            copy.start()
        for pair in range(GY_Z // 2):
            xc_ref[0, pair] = jnp.concatenate(
                [z_ref[2 * pair, :, 0:RANK], z_ref[2 * pair + 1, :, 0:RANK]], axis=1
            )
        for copy in xc_copies:
            copy.start()

    def after_x():
        for copy in xd_copies:
            copy.wait_recv()
        g_ref[0] = (xd_ref[0] + xd_ref[1]) + (xd_ref[2] + xd_ref[3])
        for copy in g_copies:
            copy.start()

    late = lax.div(GY - gy, GY)
    cross_step = CROSS_STEP + (CROSS_STEP_LATE - CROSS_STEP) * late
    first = 2 * cross_step
    high_step = HIGH_STEP - 2 * jnp.minimum(z_pos, 4)

    squares(0, 0, sq_a)

    def events(it):
        def at(when, *what):
            @pl.when(it == when)
            def _():
                for each in what:
                    each()

        def take(m):
            return functools.partial(take_values, m)

        at(1, begin)
        at(high_step, after_high)

        at(LOW_STEP, after_low)
        at(X_STEP, after_x)

        @pl.when((it >= cross_step - 1) & (it <= cross_step + 11))
        def _():
            at(cross_step - 1, take_meta)
            at(cross_step, take(0))
            at(cross_step + 3, take(1))
            at(cross_step + 4, ret_copies[0].start)
            at(cross_step + 6, take(2), ret_copies[1].start)
            at(cross_step + 8, take(3), ret_copies[2].start)
            at(cross_step + 9, take(4))
            at(cross_step + 10, take(5), ret_copies[3].start)
            at(cross_step + 11, ret_copies[4].start, ret_copies[5].start)

    def body(it, carry):
        events(it)
        before, this, second, third = carry
        position = it * 2 + 2
        coming = (second, third, pair_of(position + 1, first), pair_of(position + 2, first))
        squares(second[0], second[1], sq_b)
        tile(sq_a, hi_a, lo_a)
        uses(before, hi_b, lo_b)
        squares(third[0], third[1], sq_a)
        tile(sq_b, hi_b, lo_b)
        uses(this, hi_a, lo_a)
        return coming

    start = tuple(pair_of(jnp.int32(position), first) for position in (-1, 0, 1, 2))
    before, *_ = lax.fori_loop(0, TILES // 2, body, start)
    uses(before, hi_b, lo_b)

    loads[6].wait()
    loads[7].wait()
    top_hi[...], top_lo[...] = halves(top_ref[0])
    coup_hi[...], coup_lo[...] = halves(coup_ref[0])
    ct_halves = halves(ct_ref[0])
    for copy in xc_copies:
        copy.wait_recv()
    coupled = jnp.zeros((RHS, RANK), F32)
    for k in range(4):
        partner = clist_ref[0, k]
        used = jnp.where(partner >= 0, 1.0, 0.0)
        place = jnp.maximum(partner, 0)
        slot_z = lax.rem(z_pos + GY_Z - lax.div(place, GX_X), GY_Z)
        slot_x = lax.rem(x_pos + GX_X - lax.rem(place, GX_X), GX_X)
        row = xc_ref[slot_x, lax.div(slot_z, 2)]
        odd = lax.rem(slot_z, 2).astype(F32)
        chosen = row[:, 0:RANK] * ((1.0 - odd) * used) + row[:, RANK : 2 * RANK] * (odd * used)
        coupled = coupled + product(halves(chosen), (coup_hi[k], coup_lo[k]), mm)

    for copy in g_copies:
        copy.wait_recv()
    field = jnp.zeros((RHS, RANK), F32)
    for h in range(GX):
        slot = lax.rem(gx + GX - h, GX)
        gap = lax.max(gx - h, h - gx)
        far = jnp.where(gap >= 2, 1.0, 0.0)
        field = field + product(halves(jnp.concatenate([g_ref[slot, :, 0:RANK], g_ref[slot, :, RANK:]], axis=0) * far), (top_hi[h], top_lo[h]), mm)
    cluster = coupled + product(halves(field), ct_halves, mt)
    cluster = halves(cluster)
    for t in range(OWN):
        cols = slice(t * LEAF, (t + 1) * LEAF)
        leaf_field = product(cluster, (lt_hi[t], lt_lo[t]), mt)
        far_values = product(halves(leaf_field), (base_hi[:, cols], base_lo[:, cols]), mm)
        near_sums = acc_ref[t]
        if t >= OWN - REACH:
            ret_copies[OWN - 1 - t].wait_recv()
            near_sums = near_sums + ret_ref[OWN - 1 - t]
        out_ref[:, cols] = near_sums * OUT_SCALE + far_values

    for copy in [pts_copy, list_copy] + halo_copies + ret_copies + z_copies + xd_copies + xc_copies + g_copies:
        copy.wait_send()


def per_device(*arrays):
    rhs_values = arrays[0]
    vmem = pl.BlockSpec(memory_space=pltpu.VMEM)
    anywhere = pl.BlockSpec(memory_space=pl.ANY)
    smem = pl.BlockSpec(memory_space=pltpu.SMEM)
    dma = pltpu.SemaphoreType.DMA
    return pl.pallas_call(
        kernel,
        out_shape=jax.ShapeDtypeStruct(rhs_values.shape, F32),
        in_specs=[anywhere] * 6 + [smem] + [anywhere] * 2,
        out_specs=vmem,
        scratch_shapes=[
            pltpu.VMEM((RHS, OWN * LEAF), F32),
            pltpu.VMEM((3, OWN * LEAF), F32),
            pltpu.VMEM((RANK, OWN * LEAF), F32),
            pltpu.VMEM((OWN, RANK, RANK), F32),
            pltpu.VMEM((1, RANK, RANK), F32),
            pltpu.VMEM((OWN, NEAR), jnp.int32),
            pltpu.VMEM((1, 4, RANK, RANK), F32),
            pltpu.VMEM((1, GX, RANK, RANK), F32),
            pltpu.VMEM((OWN, RANK, RANK), BF16),
            pltpu.VMEM((OWN, RANK, RANK), BF16),
            pltpu.VMEM((GX, RANK, RANK), BF16),
            pltpu.VMEM((GX, RANK, RANK), BF16),
            pltpu.VMEM((4, RANK, RANK), BF16),
            pltpu.VMEM((4, RANK, RANK), BF16),
            dma((8,)),
            pltpu.VMEM((TABLE, 8, LEAF), F32),
            pltpu.VMEM((OWN, 8, LEAF), F32),
            pltpu.VMEM((OWN, LEAF, 128), BF16),
            pltpu.VMEM((TABLE, 2 * RHS, LEAF), BF16),
            pltpu.VMEM((TABLE, RHS, LEAF), F32),
            pltpu.VMEM((2 * REACH + 2, 2 * OWN, LEAF), F32),
            pltpu.VMEM((RANK, OWN * LEAF), BF16),
            pltpu.VMEM((RANK, OWN * LEAF), BF16),
            pltpu.VMEM((LEAF, LEAF), F32),
            pltpu.VMEM((LEAF, LEAF), F32),
            pltpu.VMEM((LEAF, LEAF), BF16),
            pltpu.VMEM((LEAF, LEAF), BF16),
            pltpu.VMEM((LEAF, LEAF), BF16),
            pltpu.VMEM((LEAF, LEAF), BF16),
            pltpu.VMEM((REACH, RHS, LEAF), F32),
            pltpu.VMEM((3, REACH * LEAF), F32),
            pltpu.VMEM((OWN, NEAR), jnp.int32),
            pltpu.VMEM((REACH, RHS, LEAF), F32),
            pltpu.VMEM((GY_Z, RHS, 2 * RANK), F32),
            pltpu.VMEM((GX_X, RHS // 2, 2 * RANK), F32),
            pltpu.VMEM((GX_X, GY_Z // 2, RHS, 2 * RANK), F32),
            pltpu.VMEM((GX, RHS // 2, 2 * RANK), F32),
            dma((REACH,)),
            dma((REACH,)),
            dma((2,)),
            dma((2,)),
            dma((REACH,)),
            dma((REACH,)),
            dma((GY_Z - 1,)),
            dma((GY_Z - 1,)),
            dma((GX_X - 1,)),
            dma((GX_X - 1,)),
            dma((GX_X - 1,)),
            dma((GX_X - 1,)),
            dma((GX - 1,)),
            dma((GX - 1,)),
        ],
        compiler_params=pltpu.CompilerParams(collective_id=0, has_side_effects=True),
        name="h2_product",
    )(*arrays)


def solution(mesh):
    return jax.shard_map(
        per_device,
        mesh=mesh,
        in_specs=(
            P(None, ("gx", "gy")),
            P(None, ("gx", "gy")),
            P(None, ("gx", "gy")),
            P(("gx", "gy"), None, None),
            P(("gx", "gy"), None, None),
            P(("gx", "gy"), None),
            P(("gx", "gy"), None),
            P(("gx", "gy"), None, None, None),
            P("gx", None, None, None),
        ),
        out_specs=P(None, ("gx", "gy")),
        check_vma=False,
    )
```

```python
import functools

import jax
import jax.numpy as jnp
from jax import lax
from jax.experimental import pallas as pl
from jax.experimental.pallas import tpu as pltpu
from jax.sharding import PartitionSpec as P

LEAF = 256
NEAR = 12
REACH = 6
OWN = 8
RHS = 32
RANK = 64
GX = 8
GY = 32
GX_X = 4
GY_Z = 8
TABLE = OWN + REACH
FEAT = 96

F32 = jnp.float32
BF16 = jnp.bfloat16
MESH = pl.DeviceIdType.MESH

TURNS = 300.0 / 6.283185307179586
SOFT = 0.0001 * TURNS * TURNS
C2 = -4.602192823044954
C1 = 9.35955760389501
C0 = -5.69072499925369
D0 = 1.6406295037196048
COS_SCALE = 0.6095221363097632
OUT_SCALE = COS_SCALE * TURNS * 0.03 * (NEAR * LEAF) ** (-0.5)
TINY = 1e-30

CROSS = 21
TILES = 56
CROSS_STEP = 5
CROSS_STEP_LATE = 7
HIGH_STEP = 6
LOW_STEP = 7
X_STEP = 10


def halves(value):
    high = value.astype(BF16)
    low = (value - high.astype(F32)).astype(BF16)
    return high, low


def thirds(value):
    high = value.astype(BF16).astype(F32)
    rest = value - high
    middle = rest.astype(BF16).astype(F32)
    low = (rest - middle).astype(BF16).astype(F32)
    return high, middle, low


def mm(left, right):
    return lax.dot_general(left, right, (((1,), (0,)), ((), ())), preferred_element_type=F32)


def mt(left, right):
    return lax.dot_general(left, right, (((1,), (1,)), ((), ())), preferred_element_type=F32)


def product(left, right, dot):
    left_high, left_low = left
    right_high, right_low = right
    return dot(left_high, right_high) + (dot(left_low, right_high) + dot(left_high, right_low))


def step_at(position, threshold):
    return lax.div(position - threshold + 64, 64)


def pair_of(position, first):
    position = jnp.minimum(jnp.maximum(position, 0), TILES - 1)
    past_self = step_at(position, OWN)
    past_first = step_at(position, first)
    past_cross = step_at(position, first + CROSS)
    crossing = past_first - past_cross
    other = past_self - crossing
    queue = lax.max(position - OWN - CROSS * past_cross + 4, 0)
    lag = 4 - lax.div(queue, 8)
    own_a = lax.rem(queue, 8)
    own_b = lax.rem(own_a + lag, 8)
    count = position - first
    halo = step_at(count, 6) + step_at(count, 11) + step_at(count, 15) + step_at(count, 18) + step_at(count, 20)
    cross_a = count - lax.div(13 * halo - halo * halo, 2)
    cross_b = OWN + halo
    at_self = 1 - past_self
    a = at_self * position + other * own_a + crossing * cross_a
    b = at_self * position + other * own_b + crossing * cross_b
    return a, b, at_self, crossing


def kernel(
    rhs_hbm,
    pts_hbm,
    basis_hbm,
    lt_hbm,
    ct_hbm,
    near_hbm,
    clist_ref,
    coup_hbm,
    top_hbm,
    out_ref,
    rhs_ref,
    pts_ref,
    basis_ref,
    lt_ref,
    ct_ref,
    near_ref,
    coup_ref,
    top_ref,
    lt_hi,
    lt_lo,
    top_hi,
    top_lo,
    coup_hi,
    coup_lo,
    load_sem,
    xy_ref,
    centre_ref,
    left_ref,
    vals_ref,
    acc_ref,
    mask_ref,
    base_hi,
    base_lo,
    sq_a,
    sq_b,
    hi_a,
    lo_a,
    hi_b,
    lo_b,
    halo_vals,
    halo_pts,
    halo_list,
    ret_ref,
    z_ref,
    xd_ref,
    xc_ref,
    g_ref,
    halo_send,
    halo_recv,
    meta_send,
    meta_recv,
    ret_send,
    ret_recv,
    z_send,
    z_recv,
    xd_send,
    xd_recv,
    xc_send,
    xc_recv,
    g_send,
    g_recv,
):
    loads = [
        pltpu.make_async_copy(src, dst, load_sem.at[i])
        for i, (src, dst) in enumerate(
            [(rhs_hbm, rhs_ref), (basis_hbm, basis_ref), (lt_hbm, lt_ref), (ct_hbm, ct_ref), (pts_hbm, pts_ref),
             (near_hbm, near_ref), (coup_hbm, coup_ref), (top_hbm, top_ref)]
        )
    ]
    for load in loads:
        load.start()

    gx = lax.axis_index("gx")
    gy = lax.axis_index("gy")
    x_pos = lax.rem(gy, GX_X)
    z_pos = lax.div(gy, GX_X)
    wrap_up = lax.div(gy + 1, GY)
    wrap_down = lax.div(GY - gy, GY)
    following = (lax.rem(gx + wrap_up, GX), lax.rem(gy + 1, GY))
    previous = (lax.rem(gx + GX - wrap_down, GX), lax.rem(gy + GY - 1, GY))
    x_peers = [(gx, z_pos * GX_X + lax.rem(x_pos + i, GX_X)) for i in range(1, GX_X)]
    z_peers = [(gx, lax.rem(z_pos + i, GY_Z) * GX_X + x_pos) for i in range(1, GY_Z)]
    g_peers = [(lax.rem(gx + i, GX), gy) for i in range(1, GX)]

    def remote(src, dst, send, recv, device):
        return pltpu.make_async_remote_copy(
            src_ref=src, dst_ref=dst, send_sem=send, recv_sem=recv, device_id=device, device_id_type=MESH
        )

    barrier = pltpu.get_barrier_semaphore()
    greeted = [previous] + x_peers + g_peers
    for device in greeted:
        pl.semaphore_signal(barrier, inc=1, device_id=device, device_id_type=MESH)
    for i in range(1, GY_Z):

        @pl.when(z_pos + i < GY_Z)
        def _(i=i):
            pl.semaphore_signal(barrier, inc=1, device_id=z_peers[i - 1], device_id_type=MESH)

    pts_copy = remote(
        pts_ref.at[:, pl.ds(2 * LEAF, REACH * LEAF)], halo_pts, meta_send.at[0], meta_recv.at[0], following
    )
    list_copy = remote(near_ref, halo_list, meta_send.at[1], meta_recv.at[1], following)
    halo_copies = [
        remote(
            rhs_ref.at[:, pl.ds((OWN - 1 - m) * LEAF, LEAF)],
            halo_vals.at[m],
            halo_send.at[m],
            halo_recv.at[m],
            following,
        )
        for m in range(REACH)
    ]
    ret_copies = [
        remote(acc_ref.at[OWN + m], ret_ref.at[m], ret_send.at[m], ret_recv.at[m], previous)
        for m in range(REACH)
    ]
    z_copies = [
        remote(z_ref.at[0], z_ref.at[i], z_send.at[i - 1], z_recv.at[i - 1], z_peers[i - 1])
        for i in range(1, GY_Z)
    ]
    xd_copies = [
        remote(xd_ref.at[0], xd_ref.at[i], xd_send.at[i - 1], xd_recv.at[i - 1], x_peers[i - 1])
        for i in range(1, GX_X)
    ]
    xc_copies = [
        remote(xc_ref.at[0], xc_ref.at[i], xc_send.at[i - 1], xc_recv.at[i - 1], x_peers[i - 1])
        for i in range(1, GX_X)
    ]
    g_copies = [
        remote(g_ref.at[0], g_ref.at[i], g_send.at[i - 1], g_recv.at[i - 1], g_peers[i - 1])
        for i in range(1, GX)
    ]

    first_leaf = (gx * GY + gy) * OWN

    def masks_from(list_value, first):
        rows = first + lax.broadcasted_iota(jnp.int32, (OWN, NEAR), 0)
        used = list_value >= 0
        found = []
        for offset in range(-REACH, REACH + 1):
            hit = jnp.where(used & (list_value == rows + offset), 1.0, 0.0)
            found.append(jnp.broadcast_to(jnp.sum(hit, axis=1, keepdims=True), (OWN, LEAF)))
        return found

    def store_values(slot, value):
        high, low = halves(value)
        vals_ref[slot, 0:RHS, :] = high
        vals_ref[slot, RHS : 2 * RHS, :] = low

    loads[0].wait()
    for t in range(OWN):
        store_values(t, rhs_ref[:, t * LEAF : (t + 1) * LEAF])
    loads[1].wait()
    high, low = halves(basis_ref[...])
    base_hi[...] = high
    base_lo[...] = low
    loads[2].wait()
    high, low = halves(lt_ref[...])
    lt_hi[...] = high
    lt_lo[...] = low
    own_coeffs = jnp.zeros((RHS, RANK), F32)
    for t in range(OWN):
        cols = slice(t * LEAF, (t + 1) * LEAF)
        both = mt(vals_ref[t], base_hi[:, cols])
        leaf_coeffs = both[0:RHS] + both[RHS:] + mt(vals_ref[t, 0:RHS, :], base_lo[:, cols])
        own_coeffs = own_coeffs + product(halves(leaf_coeffs), (lt_hi[t], lt_lo[t]), mm)
    loads[3].wait()
    own_terms = product(halves(own_coeffs), halves(ct_ref[0]), mm)
    z_ref[0, :, 0:RANK] = own_coeffs
    z_ref[0, :, RANK : 2 * RANK] = own_terms
    loads[4].wait()
    loads[5].wait()

    def begin():
        pl.semaphore_wait(barrier, len(greeted) + z_pos)
        for i in range(1, GY_Z):
            pl.when(z_pos + i >= GY_Z)(z_copies[i - 1].start)
        pts_copy.start()
        list_copy.start()
        for copy in halo_copies:
            copy.start()

    xy_ref[...] = jnp.zeros_like(xy_ref)
    for t in range(OWN):
        xy_ref[t, 0:3, :] = pts_ref[:, t * LEAF : (t + 1) * LEAF]
    acc_ref[...] = jnp.zeros_like(acc_ref)
    hi_b[...] = jnp.zeros_like(hi_b)
    lo_b[...] = jnp.zeros_like(lo_b)
    for index, found in enumerate(masks_from(near_ref[...], first_leaf)):
        mask_ref[index, 0:OWN, :] = found
    mask_ref[2 * REACH + 1] = jnp.zeros((2 * OWN, LEAF), F32)
    ones = jnp.ones((8, LEAF), F32)
    for t in range(OWN):
        points = xy_ref[t]
        centre = jnp.broadcast_to(jnp.sum(points, axis=1, keepdims=True) * (1.0 / LEAF), (8, LEAF))
        centre_ref[t] = centre
        high, middle, low = thirds((points - centre) * TURNS)
        whole = (points - centre) * TURNS
        sq_high, sq_middle, sq_low = thirds(whole * whole)
        high, middle, low = -2.0 * high, -2.0 * middle, -2.0 * low
        rows = jnp.concatenate(
            [high, high, middle, middle, high, low, ones, ones, ones, sq_high, sq_middle, sq_low,
             jnp.zeros((128 - FEAT, LEAF), F32)],
            axis=0,
        )
        left_ref[t] = rows.T.astype(BF16)

    def features(a, b):
        whole = (xy_ref[b] - centre_ref[a]) * TURNS
        high, middle, low = thirds(whole)
        sq_high, sq_middle, sq_low = thirds(whole * whole)
        return jnp.concatenate(
            [high, middle, high, middle, low, high, sq_high, sq_middle, sq_low, ones, ones, ones], axis=0
        ).astype(BF16)

    def squares(a, b, into):
        right = features(a, b)
        into[...] = mm(left_ref[a, :, 0:FEAT], right)

    def tile(source, into_hi, into_lo):
        for part in range(4):
            rows = slice(part * 64, part * 64 + 64)
            square = source[rows, :]
            safe = jnp.maximum(square, TINY)
            turns = safe * lax.rsqrt(safe)
            turns = turns - jnp.round(turns)
            q = turns * turns
            cubic = ((q + C2) * q + C1) * q + C0
            wave = D0 - q * (cubic * cubic)
            value = wave * lax.rsqrt(safe + SOFT)
            high = value.astype(BF16)
            into_hi[rows, :] = high
            into_lo[rows, :] = (value - high.astype(F32)).astype(BF16)

    def uses(pair, from_hi, from_lo):
        a, b, at_self, crossing = pair
        high, low = from_hi[...], from_lo[...]
        offset = (1 - crossing) * (b - a) + crossing * (OWN - 1 - b - a)
        row = (1 - crossing) * b + crossing * (3 * OWN - 1 - b)
        mask_b = mask_ref[REACH - offset + (REACH + 1 + offset) * at_self, pl.ds(row, 1), :]
        mask_a = mask_ref[REACH + offset, pl.ds(a, 1), :]
        vals_a = vals_ref[a]
        vals_b = vals_ref[b]
        both = mm(vals_a, high)
        sums = both[0:RHS] + both[RHS:] + mm(vals_a[0:RHS], low)
        acc_ref[b] = acc_ref[b] + sums * mask_b
        both = mt(vals_b, high)
        sums = both[0:RHS] + both[RHS:] + mt(vals_b[0:RHS], low)
        acc_ref[a] = acc_ref[a] + sums * mask_a

    def take_meta():
        pts_copy.wait_recv()
        list_copy.wait_recv()
        for m in range(REACH):
            cols = slice((REACH - 1 - m) * LEAF, (REACH - m) * LEAF)
            xy_ref[OWN + m, 0:3, :] = halo_pts[:, cols]
        for index, found in enumerate(masks_from(halo_list[...], first_leaf - OWN)):
            mask_ref[index, OWN : 2 * OWN, :] = found

    def take_values(m):
        halo_copies[m].wait_recv()
        store_values(OWN + m, halo_vals[m])

    def after_high():
        for i in range(1, GY_Z):
            pl.when(i > z_pos)(z_copies[i - 1].wait_recv)
        for i in range(1, GY_Z):
            pl.when(z_pos + i < GY_Z)(z_copies[i - 1].start)

    def after_low():
        for i in range(1, GY_Z):
            pl.when(i <= z_pos)(z_copies[i - 1].wait_recv)
        terms = z_ref[0, :, RANK : 2 * RANK]
        for i in range(1, GY_Z):
            terms = terms + z_ref[i, :, RANK : 2 * RANK]
        half = RHS // 2
        xd_ref[0] = jnp.concatenate([terms[0:half], terms[half:]], axis=1)
        for copy in xd_copies:
            copy.start()
        for pair in range(GY_Z // 2):
            xc_ref[0, pair] = jnp.concatenate(
                [z_ref[2 * pair, :, 0:RANK], z_ref[2 * pair + 1, :, 0:RANK]], axis=1
            )
        for copy in xc_copies:
            copy.start()

    def after_x():
        for copy in xd_copies:
            copy.wait_recv()
        g_ref[0] = (xd_ref[0] + xd_ref[1]) + (xd_ref[2] + xd_ref[3])
        for copy in g_copies:
            copy.start()

    late = lax.div(GY - gy, GY)
    cross_step = CROSS_STEP + (CROSS_STEP_LATE - CROSS_STEP) * late
    first = 4 * cross_step
    high_step = HIGH_STEP - jnp.minimum(z_pos, 4)

    squares(0, 0, sq_a)

    def events(it):
        def at(when, *what):
            @pl.when(it == when)
            def _():
                for each in what:
                    each()

        def take(m):
            return functools.partial(take_values, m)

        at(0, begin)
        at(high_step, after_high)
        at(LOW_STEP, after_low)
        at(X_STEP, after_x)

        @pl.when((it >= cross_step - 1) & (it <= cross_step + 6))
        def _():
            at(cross_step - 1, take_meta)
            at(cross_step, take(0))
            at(cross_step + 1, take(1))
            at(cross_step + 2, ret_copies[0].start)
            at(cross_step + 3, take(2), ret_copies[1].start)
            at(cross_step + 4, take(3), take(4), ret_copies[2].start)
            at(cross_step + 5, take(5), ret_copies[3].start)
            at(cross_step + 6, ret_copies[4].start, ret_copies[5].start)

    def body(it, carry):
        events(it)
        before, this, second, third, fourth, fifth = carry
        position = it * 4 + 4
        coming = (fourth, fifth) + tuple(pair_of(position + i, first) for i in range(1, 5))
        squares(second[0], second[1], sq_b)
        tile(sq_a, hi_a, lo_a)
        uses(before, hi_b, lo_b)
        squares(third[0], third[1], sq_a)
        tile(sq_b, hi_b, lo_b)
        uses(this, hi_a, lo_a)
        squares(fourth[0], fourth[1], sq_b)
        tile(sq_a, hi_a, lo_a)
        uses(second, hi_b, lo_b)
        squares(fifth[0], fifth[1], sq_a)
        tile(sq_b, hi_b, lo_b)
        uses(third, hi_a, lo_a)
        return coming

    start = tuple(pair_of(jnp.int32(position), first) for position in range(-1, 5))
    before, *_ = lax.fori_loop(0, TILES // 4, body, start)
    uses(before, hi_b, lo_b)

    loads[6].wait()
    loads[7].wait()
    top_hi[...], top_lo[...] = halves(top_ref[0])
    coup_hi[...], coup_lo[...] = halves(coup_ref[0])
    ct_halves = halves(ct_ref[0])
    for copy in xc_copies:
        copy.wait_recv()
    coupled = jnp.zeros((RHS, RANK), F32)
    for k in range(4):
        partner = clist_ref[0, k]
        used = jnp.where(partner >= 0, 1.0, 0.0)
        place = jnp.maximum(partner, 0)
        slot_z = lax.rem(z_pos + GY_Z - lax.div(place, GX_X), GY_Z)
        slot_x = lax.rem(x_pos + GX_X - lax.rem(place, GX_X), GX_X)
        row = xc_ref[slot_x, lax.div(slot_z, 2)]
        odd = lax.rem(slot_z, 2).astype(F32)
        chosen = row[:, 0:RANK] * ((1.0 - odd) * used) + row[:, RANK : 2 * RANK] * (odd * used)
        coupled = coupled + product(halves(chosen), (coup_hi[k], coup_lo[k]), mm)

    for copy in g_copies:
        copy.wait_recv()
    field = jnp.zeros((RHS, RANK), F32)
    for h in range(GX):
        slot = lax.rem(gx + GX - h, GX)
        gap = lax.max(gx - h, h - gx)
        far = jnp.where(gap >= 2, 1.0, 0.0)
        field = field + product(halves(jnp.concatenate([g_ref[slot, :, 0:RANK], g_ref[slot, :, RANK:]], axis=0) * far), (top_hi[h], top_lo[h]), mm)
    cluster = coupled + product(halves(field), ct_halves, mt)
    cluster = halves(cluster)
    for t in range(OWN):
        cols = slice(t * LEAF, (t + 1) * LEAF)
        leaf_field = product(cluster, (lt_hi[t], lt_lo[t]), mt)
        far_values = product(halves(leaf_field), (base_hi[:, cols], base_lo[:, cols]), mm)
        near_sums = acc_ref[t]
        if t >= OWN - REACH:
            ret_copies[OWN - 1 - t].wait_recv()
            near_sums = near_sums + ret_ref[OWN - 1 - t]
        out_ref[:, cols] = near_sums * OUT_SCALE + far_values

    for copy in [pts_copy, list_copy] + halo_copies + ret_copies + z_copies + xd_copies + xc_copies + g_copies:
        copy.wait_send()


def per_device(*arrays):
    rhs_values = arrays[0]
    vmem = pl.BlockSpec(memory_space=pltpu.VMEM)
    anywhere = pl.BlockSpec(memory_space=pl.ANY)
    smem = pl.BlockSpec(memory_space=pltpu.SMEM)
    dma = pltpu.SemaphoreType.DMA
    return pl.pallas_call(
        kernel,
        out_shape=jax.ShapeDtypeStruct(rhs_values.shape, F32),
        in_specs=[anywhere] * 6 + [smem] + [anywhere] * 2,
        out_specs=vmem,
        scratch_shapes=[
            pltpu.VMEM((RHS, OWN * LEAF), F32),
            pltpu.VMEM((3, OWN * LEAF), F32),
            pltpu.VMEM((RANK, OWN * LEAF), F32),
            pltpu.VMEM((OWN, RANK, RANK), F32),
            pltpu.VMEM((1, RANK, RANK), F32),
            pltpu.VMEM((OWN, NEAR), jnp.int32),
            pltpu.VMEM((1, 4, RANK, RANK), F32),
            pltpu.VMEM((1, GX, RANK, RANK), F32),
            pltpu.VMEM((OWN, RANK, RANK), BF16),
            pltpu.VMEM((OWN, RANK, RANK), BF16),
            pltpu.VMEM((GX, RANK, RANK), BF16),
            pltpu.VMEM((GX, RANK, RANK), BF16),
            pltpu.VMEM((4, RANK, RANK), BF16),
            pltpu.VMEM((4, RANK, RANK), BF16),
            dma((8,)),
            pltpu.VMEM((TABLE, 8, LEAF), F32),
            pltpu.VMEM((OWN, 8, LEAF), F32),
            pltpu.VMEM((OWN, LEAF, 128), BF16),
            pltpu.VMEM((TABLE, 2 * RHS, LEAF), BF16),
            pltpu.VMEM((TABLE, RHS, LEAF), F32),
            pltpu.VMEM((2 * REACH + 2, 2 * OWN, LEAF), F32),
            pltpu.VMEM((RANK, OWN * LEAF), BF16),
            pltpu.VMEM((RANK, OWN * LEAF), BF16),
            pltpu.VMEM((LEAF, LEAF), F32),
            pltpu.VMEM((LEAF, LEAF), F32),
            pltpu.VMEM((LEAF, LEAF), BF16),
            pltpu.VMEM((LEAF, LEAF), BF16),
            pltpu.VMEM((LEAF, LEAF), BF16),
            pltpu.VMEM((LEAF, LEAF), BF16),
            pltpu.VMEM((REACH, RHS, LEAF), F32),
            pltpu.VMEM((3, REACH * LEAF), F32),
            pltpu.VMEM((OWN, NEAR), jnp.int32),
            pltpu.VMEM((REACH, RHS, LEAF), F32),
            pltpu.VMEM((GY_Z, RHS, 2 * RANK), F32),
            pltpu.VMEM((GX_X, RHS // 2, 2 * RANK), F32),
            pltpu.VMEM((GX_X, GY_Z // 2, RHS, 2 * RANK), F32),
            pltpu.VMEM((GX, RHS // 2, 2 * RANK), F32),
            dma((REACH,)),
            dma((REACH,)),
            dma((2,)),
            dma((2,)),
            dma((REACH,)),
            dma((REACH,)),
            dma((GY_Z - 1,)),
            dma((GY_Z - 1,)),
            dma((GX_X - 1,)),
            dma((GX_X - 1,)),
            dma((GX_X - 1,)),
            dma((GX_X - 1,)),
            dma((GX - 1,)),
            dma((GX - 1,)),
        ],
        compiler_params=pltpu.CompilerParams(collective_id=0, has_side_effects=True),
        name="h2_product",
    )(*arrays)


def solution(mesh):
    return jax.shard_map(
        per_device,
        mesh=mesh,
        in_specs=(
            P(None, ("gx", "gy")),
            P(None, ("gx", "gy")),
            P(None, ("gx", "gy")),
            P(("gx", "gy"), None, None),
            P(("gx", "gy"), None, None),
            P(("gx", "gy"), None),
            P(("gx", "gy"), None),
            P(("gx", "gy"), None, None, None),
            P("gx", None, None, None),
        ),
        out_specs=P(None, ("gx", "gy")),
        check_vma=False,
    )
```

```python
import functools

import jax
import jax.numpy as jnp
from jax import lax
from jax.experimental import pallas as pl
from jax.experimental.pallas import tpu as pltpu
from jax.sharding import PartitionSpec as P

LEAF = 256
NEAR = 12
REACH = 6
OWN = 8
RHS = 32
RANK = 64
GX = 8
GY = 32
GX_X = 4
GY_Z = 8
TABLE = OWN + REACH
FEAT = 96

F32 = jnp.float32
BF16 = jnp.bfloat16
MESH = pl.DeviceIdType.MESH

TURNS = 300.0 / 6.283185307179586
SOFT = 0.0001 * TURNS * TURNS
C2 = -4.602192823044954
C1 = 9.35955760389501
C0 = -5.69072499925369
D0 = 1.6406295037196048
COS_SCALE = 0.6095221363097632
OUT_SCALE = COS_SCALE * TURNS * 0.03 * (NEAR * LEAF) ** (-0.5)
TINY = 1e-30

CROSS = 21
TILES = 56
CROSS_STEP = 5
CROSS_STEP_LATE = 8
HIGH_STEP = 6
LOW_STEP = 7
X_STEP = 10


def halves(value):
    high = value.astype(BF16)
    low = (value - high.astype(F32)).astype(BF16)
    return high, low


def thirds(value):
    high = value.astype(BF16).astype(F32)
    rest = value - high
    middle = rest.astype(BF16).astype(F32)
    low = (rest - middle).astype(BF16).astype(F32)
    return high, middle, low


def mm(left, right):
    return lax.dot_general(left, right, (((1,), (0,)), ((), ())), preferred_element_type=F32)


def mt(left, right):
    return lax.dot_general(left, right, (((1,), (1,)), ((), ())), preferred_element_type=F32)


def product(left, right, dot):
    left_high, left_low = left
    right_high, right_low = right
    return dot(left_high, right_high) + (dot(left_low, right_high) + dot(left_high, right_low))


def step_at(position, threshold):
    return lax.div(position - threshold + 64, 64)


def pair_of(position, first):
    position = jnp.minimum(jnp.maximum(position, 0), TILES - 1)
    past_self = step_at(position, OWN)
    past_first = step_at(position, first)
    past_cross = step_at(position, first + CROSS)
    crossing = past_first - past_cross
    other = past_self - crossing
    queue = lax.max(position - OWN - CROSS * past_cross + 4, 0)
    lag = 4 - lax.div(queue, 8)
    own_a = lax.rem(queue, 8)
    own_b = lax.rem(own_a + lag, 8)
    count = position - first
    halo = step_at(count, 6) + step_at(count, 11) + step_at(count, 15) + step_at(count, 18) + step_at(count, 20)
    cross_a = count - lax.div(13 * halo - halo * halo, 2)
    cross_b = OWN + halo
    at_self = 1 - past_self
    a = at_self * position + other * own_a + crossing * cross_a
    b = at_self * position + other * own_b + crossing * cross_b
    return a, b, at_self, crossing


def kernel(
    rhs_hbm,
    pts_hbm,
    basis_hbm,
    lt_hbm,
    ct_hbm,
    near_hbm,
    clist_ref,
    coup_hbm,
    top_hbm,
    out_ref,
    rhs_ref,
    pts_ref,
    basis_ref,
    lt_ref,
    ct_ref,
    near_ref,
    coup_ref,
    top_ref,
    lt_hi,
    lt_lo,
    top_hi,
    top_lo,
    coup_hi,
    coup_lo,
    load_sem,
    xy_ref,
    centre_ref,
    left_ref,
    vals_ref,
    acc_ref,
    mask_ref,
    base_hi,
    base_lo,
    sq_a,
    sq_b,
    hi_a,
    lo_a,
    hi_b,
    lo_b,
    halo_vals,
    halo_pts,
    halo_list,
    ret_ref,
    z_ref,
    xd_ref,
    xc_ref,
    g_ref,
    halo_send,
    halo_recv,
    meta_send,
    meta_recv,
    ret_send,
    ret_recv,
    z_send,
    z_recv,
    xd_send,
    xd_recv,
    xc_send,
    xc_recv,
    g_send,
    g_recv,
):
    loads = [
        pltpu.make_async_copy(src, dst, load_sem.at[i])
        for i, (src, dst) in enumerate(
            [(rhs_hbm, rhs_ref), (basis_hbm, basis_ref), (lt_hbm, lt_ref), (ct_hbm, ct_ref), (pts_hbm, pts_ref),
             (near_hbm, near_ref), (coup_hbm, coup_ref), (top_hbm, top_ref)]
        )
    ]
    for load in loads:
        load.start()

    gx = lax.axis_index("gx")
    gy = lax.axis_index("gy")
    x_pos = lax.rem(gy, GX_X)
    z_pos = lax.div(gy, GX_X)
    wrap_up = lax.div(gy + 1, GY)
    wrap_down = lax.div(GY - gy, GY)
    following = (lax.rem(gx + wrap_up, GX), lax.rem(gy + 1, GY))
    previous = (lax.rem(gx + GX - wrap_down, GX), lax.rem(gy + GY - 1, GY))
    x_peers = [(gx, z_pos * GX_X + lax.rem(x_pos + i, GX_X)) for i in range(1, GX_X)]
    z_peers = [(gx, lax.rem(z_pos + i, GY_Z) * GX_X + x_pos) for i in range(1, GY_Z)]
    g_peers = [(lax.rem(gx + i, GX), gy) for i in range(1, GX)]

    def remote(src, dst, send, recv, device):
        return pltpu.make_async_remote_copy(
            src_ref=src, dst_ref=dst, send_sem=send, recv_sem=recv, device_id=device, device_id_type=MESH
        )

    barrier = pltpu.get_barrier_semaphore()
    greeted = [previous] + x_peers + g_peers
    for device in greeted:
        pl.semaphore_signal(barrier, inc=1, device_id=device, device_id_type=MESH)
    for i in range(1, GY_Z):

        @pl.when(z_pos + i < GY_Z)
        def _(i=i):
            pl.semaphore_signal(barrier, inc=1, device_id=z_peers[i - 1], device_id_type=MESH)

    pts_copy = remote(
        pts_ref.at[:, pl.ds(2 * LEAF, REACH * LEAF)], halo_pts, meta_send.at[0], meta_recv.at[0], following
    )
    list_copy = remote(near_ref, halo_list, meta_send.at[1], meta_recv.at[1], following)
    halo_copies = [
        remote(
            rhs_ref.at[:, pl.ds((OWN - 1 - m) * LEAF, LEAF)],
            halo_vals.at[m],
            halo_send.at[m],
            halo_recv.at[m],
            following,
        )
        for m in range(REACH)
    ]
    ret_copies = [
        remote(acc_ref.at[OWN + m], ret_ref.at[m], ret_send.at[m], ret_recv.at[m], previous)
        for m in range(REACH)
    ]
    z_copies = [
        remote(z_ref.at[0], z_ref.at[i], z_send.at[i - 1], z_recv.at[i - 1], z_peers[i - 1])
        for i in range(1, GY_Z)
    ]
    xd_copies = [
        remote(xd_ref.at[0], xd_ref.at[i], xd_send.at[i - 1], xd_recv.at[i - 1], x_peers[i - 1])
        for i in range(1, GX_X)
    ]
    xc_copies = [
        remote(xc_ref.at[0], xc_ref.at[i], xc_send.at[i - 1], xc_recv.at[i - 1], x_peers[i - 1])
        for i in range(1, GX_X)
    ]
    g_copies = [
        remote(g_ref.at[0], g_ref.at[i], g_send.at[i - 1], g_recv.at[i - 1], g_peers[i - 1])
        for i in range(1, GX)
    ]

    first_leaf = (gx * GY + gy) * OWN

    def masks_from(list_value, first):
        rows = first + lax.broadcasted_iota(jnp.int32, (OWN, NEAR), 0)
        used = list_value >= 0
        found = []
        for offset in range(-REACH, REACH + 1):
            hit = jnp.where(used & (list_value == rows + offset), 1.0, 0.0)
            found.append(jnp.broadcast_to(jnp.sum(hit, axis=1, keepdims=True), (OWN, LEAF)))
        return found

    def store_values(slot, value):
        high, low = halves(value)
        vals_ref[slot, 0:RHS, :] = high
        vals_ref[slot, RHS : 2 * RHS, :] = low

    loads[0].wait()
    for t in range(OWN):
        store_values(t, rhs_ref[:, t * LEAF : (t + 1) * LEAF])
    loads[1].wait()
    high, low = halves(basis_ref[...])
    base_hi[...] = high
    base_lo[...] = low
    loads[2].wait()
    high, low = halves(lt_ref[...])
    lt_hi[...] = high
    lt_lo[...] = low
    own_coeffs = jnp.zeros((RHS, RANK), F32)
    for t in range(OWN):
        cols = slice(t * LEAF, (t + 1) * LEAF)
        both = mt(vals_ref[t], base_hi[:, cols])
        leaf_coeffs = both[0:RHS] + both[RHS:] + mt(vals_ref[t, 0:RHS, :], base_lo[:, cols])
        own_coeffs = own_coeffs + product(halves(leaf_coeffs), (lt_hi[t], lt_lo[t]), mm)
    loads[3].wait()
    own_terms = product(halves(own_coeffs), halves(ct_ref[0]), mm)
    z_ref[0, :, 0:RANK] = own_coeffs
    z_ref[0, :, RANK : 2 * RANK] = own_terms
    loads[4].wait()
    loads[5].wait()

    def begin():
        pl.semaphore_wait(barrier, len(greeted) + z_pos)
        for i in range(1, GY_Z):
            pl.when(z_pos + i >= GY_Z)(z_copies[i - 1].start)
        pts_copy.start()
        list_copy.start()
        for copy in halo_copies:
            copy.start()

    xy_ref[...] = jnp.zeros_like(xy_ref)
    for t in range(OWN):
        xy_ref[t, 0:3, :] = pts_ref[:, t * LEAF : (t + 1) * LEAF]
    acc_ref[...] = jnp.zeros_like(acc_ref)
    hi_b[...] = jnp.zeros_like(hi_b)
    lo_b[...] = jnp.zeros_like(lo_b)
    for index, found in enumerate(masks_from(near_ref[...], first_leaf)):
        mask_ref[index, 0:OWN, :] = found
    mask_ref[2 * REACH + 1] = jnp.zeros((2 * OWN, LEAF), F32)
    ones = jnp.ones((8, LEAF), F32)
    for t in range(OWN):
        points = xy_ref[t]
        centre = jnp.broadcast_to(jnp.sum(points, axis=1, keepdims=True) * (1.0 / LEAF), (8, LEAF))
        centre_ref[t] = centre
        high, middle, low = thirds((points - centre) * TURNS)
        whole = (points - centre) * TURNS
        sq_high, sq_middle, sq_low = thirds(whole * whole)
        high, middle, low = -2.0 * high, -2.0 * middle, -2.0 * low
        rows = jnp.concatenate(
            [high, high, middle, middle, high, low, ones, ones, ones, sq_high, sq_middle, sq_low,
             jnp.zeros((128 - FEAT, LEAF), F32)],
            axis=0,
        )
        left_ref[t] = rows.T.astype(BF16)

    def features(a, b):
        whole = (xy_ref[b] - centre_ref[a]) * TURNS
        high, middle, low = thirds(whole)
        sq_high, sq_middle, sq_low = thirds(whole * whole)
        return jnp.concatenate(
            [high, middle, high, middle, low, high, sq_high, sq_middle, sq_low, ones, ones, ones], axis=0
        ).astype(BF16)

    def squares(a, b, into):
        right = features(a, b)
        into[...] = mm(left_ref[a, :, 0:FEAT], right)

    def tile(source, into_hi, into_lo):
        for part in range(4):
            rows = slice(part * 64, part * 64 + 64)
            square = source[rows, :]
            safe = jnp.maximum(square, TINY)
            turns = safe * lax.rsqrt(safe)
            turns = turns - jnp.round(turns)
            q = turns * turns
            cubic = ((q + C2) * q + C1) * q + C0
            wave = D0 - q * (cubic * cubic)
            value = wave * lax.rsqrt(safe + SOFT)
            high = value.astype(BF16)
            into_hi[rows, :] = high
            into_lo[rows, :] = (value - high.astype(F32)).astype(BF16)

    def uses(pair, from_hi, from_lo):
        a, b, at_self, crossing = pair
        high, low = from_hi[...], from_lo[...]
        offset = (1 - crossing) * (b - a) + crossing * (OWN - 1 - b - a)
        row = (1 - crossing) * b + crossing * (3 * OWN - 1 - b)
        mask_b = mask_ref[REACH - offset + (REACH + 1 + offset) * at_self, pl.ds(row, 1), :]
        mask_a = mask_ref[REACH + offset, pl.ds(a, 1), :]
        vals_a = vals_ref[a]
        vals_b = vals_ref[b]
        both = mm(vals_a, high)
        sums = both[0:RHS] + both[RHS:] + mm(vals_a[0:RHS], low)
        acc_ref[b] = acc_ref[b] + sums * mask_b
        both = mt(vals_b, high)
        sums = both[0:RHS] + both[RHS:] + mt(vals_b[0:RHS], low)
        acc_ref[a] = acc_ref[a] + sums * mask_a

    def take_meta():
        pts_copy.wait_recv()
        list_copy.wait_recv()
        for m in range(REACH):
            cols = slice((REACH - 1 - m) * LEAF, (REACH - m) * LEAF)
            xy_ref[OWN + m, 0:3, :] = halo_pts[:, cols]
        for index, found in enumerate(masks_from(halo_list[...], first_leaf - OWN)):
            mask_ref[index, OWN : 2 * OWN, :] = found

    def take_values(m):
        halo_copies[m].wait_recv()
        store_values(OWN + m, halo_vals[m])

    def after_high():
        for i in range(1, GY_Z):
            pl.when(i > z_pos)(z_copies[i - 1].wait_recv)
        for i in range(1, GY_Z):
            pl.when(z_pos + i < GY_Z)(z_copies[i - 1].start)

    def after_low():
        for i in range(1, GY_Z):
            pl.when(i <= z_pos)(z_copies[i - 1].wait_recv)
        terms = z_ref[0, :, RANK : 2 * RANK]
        for i in range(1, GY_Z):
            terms = terms + z_ref[i, :, RANK : 2 * RANK]
        half = RHS // 2
        xd_ref[0] = jnp.concatenate([terms[0:half], terms[half:]], axis=1)
        for copy in xd_copies:
            copy.start()
        for pair in range(GY_Z // 2):
            xc_ref[0, pair] = jnp.concatenate(
                [z_ref[2 * pair, :, 0:RANK], z_ref[2 * pair + 1, :, 0:RANK]], axis=1
            )
        for copy in xc_copies:
            copy.start()

    def after_x():
        for copy in xd_copies:
            copy.wait_recv()
        g_ref[0] = (xd_ref[0] + xd_ref[1]) + (xd_ref[2] + xd_ref[3])
        for copy in g_copies:
            copy.start()

    late = lax.div(GY - gy, GY)
    cross_step = CROSS_STEP + (CROSS_STEP_LATE - CROSS_STEP) * late
    first = 4 * cross_step
    begin_step = 1 - lax.div(jnp.minimum(z_pos, 4), 4)
    high_step = HIGH_STEP - jnp.minimum(z_pos, 4)

    squares(0, 0, sq_a)

    def events(it):
        def at(when, *what):
            @pl.when(it == when)
            def _():
                for each in what:
                    each()

        def take(m):
            return functools.partial(take_values, m)

        at(begin_step, begin)
        at(high_step, after_high)
        at(LOW_STEP, after_low)
        at(X_STEP, after_x)

        @pl.when((it >= cross_step - 1) & (it <= cross_step + 6))
        def _():
            at(cross_step - 1, take_meta)
            at(cross_step, take(0))
            at(cross_step + 1, take(1))
            at(cross_step + 2, ret_copies[0].start)
            at(cross_step + 3, take(2), ret_copies[1].start)
            at(cross_step + 4, take(3), take(4), ret_copies[2].start)
            at(cross_step + 5, take(5), ret_copies[3].start)
            at(cross_step + 6, ret_copies[4].start, ret_copies[5].start)

    def body(it, carry):
        events(it)
        before, this, second, third, fourth, fifth = carry
        position = it * 4 + 4
        coming = (fourth, fifth) + tuple(pair_of(position + i, first) for i in range(1, 5))
        squares(second[0], second[1], sq_b)
        tile(sq_a, hi_a, lo_a)
        uses(before, hi_b, lo_b)
        squares(third[0], third[1], sq_a)
        tile(sq_b, hi_b, lo_b)
        uses(this, hi_a, lo_a)
        squares(fourth[0], fourth[1], sq_b)
        tile(sq_a, hi_a, lo_a)
        uses(second, hi_b, lo_b)
        squares(fifth[0], fifth[1], sq_a)
        tile(sq_b, hi_b, lo_b)
        uses(third, hi_a, lo_a)
        return coming

    start = tuple(pair_of(jnp.int32(position), first) for position in range(-1, 5))
    before, *_ = lax.fori_loop(0, TILES // 4, body, start)
    uses(before, hi_b, lo_b)

    @pl.when(cross_step + 6 >= TILES // 4)
    def _():
        ret_copies[4].start()
        ret_copies[5].start()

    loads[6].wait()
    loads[7].wait()
    top_hi[...], top_lo[...] = halves(top_ref[0])
    coup_hi[...], coup_lo[...] = halves(coup_ref[0])
    ct_halves = halves(ct_ref[0])
    for copy in xc_copies:
        copy.wait_recv()
    coupled = jnp.zeros((RHS, RANK), F32)
    for k in range(4):
        partner = clist_ref[0, k]
        used = jnp.where(partner >= 0, 1.0, 0.0)
        place = jnp.maximum(partner, 0)
        slot_z = lax.rem(z_pos + GY_Z - lax.div(place, GX_X), GY_Z)
        slot_x = lax.rem(x_pos + GX_X - lax.rem(place, GX_X), GX_X)
        row = xc_ref[slot_x, lax.div(slot_z, 2)]
        odd = lax.rem(slot_z, 2).astype(F32)
        chosen = row[:, 0:RANK] * ((1.0 - odd) * used) + row[:, RANK : 2 * RANK] * (odd * used)
        coupled = coupled + product(halves(chosen), (coup_hi[k], coup_lo[k]), mm)

    for copy in g_copies:
        copy.wait_recv()
    field = jnp.zeros((RHS, RANK), F32)
    for h in range(GX):
        slot = lax.rem(gx + GX - h, GX)
        gap = lax.max(gx - h, h - gx)
        far = jnp.where(gap >= 2, 1.0, 0.0)
        field = field + product(halves(jnp.concatenate([g_ref[slot, :, 0:RANK], g_ref[slot, :, RANK:]], axis=0) * far), (top_hi[h], top_lo[h]), mm)
    cluster = coupled + product(halves(field), ct_halves, mt)
    cluster = halves(cluster)
    for t in range(OWN):
        cols = slice(t * LEAF, (t + 1) * LEAF)
        leaf_field = product(cluster, (lt_hi[t], lt_lo[t]), mt)
        far_values = product(halves(leaf_field), (base_hi[:, cols], base_lo[:, cols]), mm)
        near_sums = acc_ref[t]
        if t >= OWN - REACH:
            ret_copies[OWN - 1 - t].wait_recv()
            near_sums = near_sums + ret_ref[OWN - 1 - t]
        out_ref[:, cols] = near_sums * OUT_SCALE + far_values

    for copy in [pts_copy, list_copy] + halo_copies + ret_copies + z_copies + xd_copies + xc_copies + g_copies:
        copy.wait_send()


def per_device(*arrays):
    rhs_values = arrays[0]
    vmem = pl.BlockSpec(memory_space=pltpu.VMEM)
    anywhere = pl.BlockSpec(memory_space=pl.ANY)
    smem = pl.BlockSpec(memory_space=pltpu.SMEM)
    dma = pltpu.SemaphoreType.DMA
    return pl.pallas_call(
        kernel,
        out_shape=jax.ShapeDtypeStruct(rhs_values.shape, F32),
        in_specs=[anywhere] * 6 + [smem] + [anywhere] * 2,
        out_specs=vmem,
        scratch_shapes=[
            pltpu.VMEM((RHS, OWN * LEAF), F32),
            pltpu.VMEM((3, OWN * LEAF), F32),
            pltpu.VMEM((RANK, OWN * LEAF), F32),
            pltpu.VMEM((OWN, RANK, RANK), F32),
            pltpu.VMEM((1, RANK, RANK), F32),
            pltpu.VMEM((OWN, NEAR), jnp.int32),
            pltpu.VMEM((1, 4, RANK, RANK), F32),
            pltpu.VMEM((1, GX, RANK, RANK), F32),
            pltpu.VMEM((OWN, RANK, RANK), BF16),
            pltpu.VMEM((OWN, RANK, RANK), BF16),
            pltpu.VMEM((GX, RANK, RANK), BF16),
            pltpu.VMEM((GX, RANK, RANK), BF16),
            pltpu.VMEM((4, RANK, RANK), BF16),
            pltpu.VMEM((4, RANK, RANK), BF16),
            dma((8,)),
            pltpu.VMEM((TABLE, 8, LEAF), F32),
            pltpu.VMEM((OWN, 8, LEAF), F32),
            pltpu.VMEM((OWN, LEAF, 128), BF16),
            pltpu.VMEM((TABLE, 2 * RHS, LEAF), BF16),
            pltpu.VMEM((TABLE, RHS, LEAF), F32),
            pltpu.VMEM((2 * REACH + 2, 2 * OWN, LEAF), F32),
            pltpu.VMEM((RANK, OWN * LEAF), BF16),
            pltpu.VMEM((RANK, OWN * LEAF), BF16),
            pltpu.VMEM((LEAF, LEAF), F32),
            pltpu.VMEM((LEAF, LEAF), F32),
            pltpu.VMEM((LEAF, LEAF), BF16),
            pltpu.VMEM((LEAF, LEAF), BF16),
            pltpu.VMEM((LEAF, LEAF), BF16),
            pltpu.VMEM((LEAF, LEAF), BF16),
            pltpu.VMEM((REACH, RHS, LEAF), F32),
            pltpu.VMEM((3, REACH * LEAF), F32),
            pltpu.VMEM((OWN, NEAR), jnp.int32),
            pltpu.VMEM((REACH, RHS, LEAF), F32),
            pltpu.VMEM((GY_Z, RHS, 2 * RANK), F32),
            pltpu.VMEM((GX_X, RHS // 2, 2 * RANK), F32),
            pltpu.VMEM((GX_X, GY_Z // 2, RHS, 2 * RANK), F32),
            pltpu.VMEM((GX, RHS // 2, 2 * RANK), F32),
            dma((REACH,)),
            dma((REACH,)),
            dma((2,)),
            dma((2,)),
            dma((REACH,)),
            dma((REACH,)),
            dma((GY_Z - 1,)),
            dma((GY_Z - 1,)),
            dma((GX_X - 1,)),
            dma((GX_X - 1,)),
            dma((GX_X - 1,)),
            dma((GX_X - 1,)),
            dma((GX - 1,)),
            dma((GX - 1,)),
        ],
        compiler_params=pltpu.CompilerParams(collective_id=0, has_side_effects=True),
        name="h2_product",
    )(*arrays)


def solution(mesh):
    return jax.shard_map(
        per_device,
        mesh=mesh,
        in_specs=(
            P(None, ("gx", "gy")),
            P(None, ("gx", "gy")),
            P(None, ("gx", "gy")),
            P(("gx", "gy"), None, None),
            P(("gx", "gy"), None, None),
            P(("gx", "gy"), None),
            P(("gx", "gy"), None),
            P(("gx", "gy"), None, None, None),
            P("gx", None, None, None),
        ),
        out_specs=P(None, ("gx", "gy")),
        check_vma=False,
    )
```
